32 devices in a mesh: section: 4 (over y, x), dp: 8 (over z, core).
Axes of the slice: x: 2, y: 2, z: 4, core: 2. Of those that a mesh axis runs over, the one named last changes fastest.
Arguments:
- activations: bfloat16 [4, 8, 257, 1792], P('section', 'dp'), may hold values from -6 to 6
- saved: bfloat16 [4, 8, 257, 1792], P('section', 'dp'), may hold values from -6 to 6
- cotangents: bfloat16 [4, 8, 257, 1792], P('section', 'dp'), may hold values from -1.1953125 to 1.1953125
- projection: bfloat16 [4, 1792, 1792], P('section'), may hold values from -0.125 to 0.125
- section_gain: float32 [4, 1792], P('section'), may hold values from 0.5 to 1.5
- final_gain: float32 [1792], replicated, may hold values from 0.5 to 1.5
- head_weight: bfloat16 [1792, 1024], P('section'), may hold values from -0.125 to 0.125
- text_embed: bfloat16 [8, 1024], P('dp'), may hold values from -6 to 6
- labels: int32 [8], P('dp'), may hold values from 0 to 7, each once
Outputs:
- next_act: bfloat16 [4, 8, 257, 1792], P('section', 'dp')
- next_grad: bfloat16 [4, 8, 257, 1792], P('section', 'dp')
- mean_loss: float32 [4], P('section')
The draws below stay inside these ranges and needn't reach their ends.
Inputs may be any that keep to these rules, and one draw needn't show every extreme that they name: labels holds each caption index once.
All inputs are finite; a program needn't handle non-finite values.
Results may differ from the reference program's by a relative error of at most 0.0039.
Values may be sent and summed in bfloat16 or wider, within the bound.
A program may use at most 64 MiB of HBM per device.

```python
import jax
import jax.numpy as jnp
from jax import lax

D = 1792
E = 1024
TOK = 257
B = 8
N_SECTION = 4


def block_scale(key, extent, split, low, high):
    def one(position, shards_of):
        draws = jax.random.uniform(jax.random.fold_in(jax.random.fold_in(key, 6), position), (shards_of,), jnp.float32, low / len(split), high / len(split))
        return jnp.repeat(jnp.exp(draws), extent[position] // shards_of).reshape((-1,) + (1,) * (len(extent) - position - 1))

    factor_of = one(*split[0])
    for cut in split[1:]:
        factor_of = factor_of * one(*cut)
    return factor_of


def noise(key, dims, width, most, cuts=(), held_as=jnp.bfloat16):
    array = width * jax.random.normal(key, dims, jnp.float32)
    if cuts:
        array = array * block_scale(key, dims, cuts, -0.22, 0.18)
    return jnp.clip(array, -most, most).astype(held_as)


def setup_inputs(seed: int = 0) -> dict:
    arg_keys = jax.random.split(jax.random.key(seed), 10)
    return {
        "activations": noise(arg_keys[0], (N_SECTION, B, TOK, D), 1.0, 6.0, ((0, 4), (1, 8))),
        "saved": noise(arg_keys[1], (N_SECTION, B, TOK, D), 1.0, 6.0, ((0, 4), (1, 8))),
        "cotangents": noise(arg_keys[2], (N_SECTION, B, TOK, D), 0.2, 1.1953125, ((0, 4), (1, 8))),
        "projection": noise(arg_keys[3], (N_SECTION, D, D), D ** -0.5, 0.125, ((0, 4),)),
        "section_gain": jnp.clip(1.0 + 0.1 * jax.random.normal(arg_keys[4], (N_SECTION, D), jnp.float32), 0.5, 1.5),
        "final_gain": jnp.clip(1.0 + 0.1 * jax.random.normal(arg_keys[5], (D,), jnp.float32), 0.5, 1.5),
        "head_weight": noise(arg_keys[6], (D, E), D ** -0.5, 0.125, ((0, 4),)),
        "text_embed": noise(arg_keys[7], (B, E), 1.0, 6.0, ((0, 8),)),
        "labels": jax.random.permutation(arg_keys[8], B).astype(jnp.int32),
    }


epsilon = 1e-06
logit_scale = 100.0

def norm_rows(values):
    centre = lax.optimization_barrier(jnp.mean(values, axis=-1, keepdims=True))
    centred = values - centre
    variance = lax.optimization_barrier(jnp.mean(centred * centred, axis=-1, keepdims=True))
    inverse = lax.rsqrt(variance + epsilon)
    return (centred * inverse, inverse)

def unit_rows(values):
    inverse = lax.rsqrt(lax.optimization_barrier(jnp.sum(values * values, axis=-1, keepdims=True)) + epsilon)
    return (values * inverse, inverse)

def forward_block(block_in, weight, scale_row):
    block_shape = block_in.shape
    standard, inverse = norm_rows(block_in.astype(jnp.float32))
    normed = (standard * scale_row).astype(jnp.bfloat16)
    mixed = jnp.dot(normed.reshape(-1, block_shape[-1]), weight, preferred_element_type=jnp.float32)
    return (block_in.astype(jnp.float32) + mixed.reshape(block_shape)).astype(jnp.bfloat16)

def backward_block(cotangent, restored, weight, scale_row):
    block_shape = restored.shape
    standard, inverse = norm_rows(restored.astype(jnp.float32))
    d_normed = lax.dot_general(cotangent.reshape(-1, block_shape[-1]), weight, (((1,), (1,)), ((), ())), preferred_element_type=jnp.float32).reshape(block_shape)
    d_standard = d_normed * scale_row
    d_input = cotangent.astype(jnp.float32) + inverse * (d_standard - lax.optimization_barrier(jnp.mean(d_standard, axis=-1, keepdims=True)) - standard * lax.optimization_barrier(jnp.mean(d_standard * standard, axis=-1, keepdims=True)))
    return d_input.astype(jnp.bfloat16)

def reference(activations, saved, cotangents, projection, section_gain, final_gain, head_weight, text_embed, labels):
    block_out = lax.map(lambda item: forward_block(item[0], item[1], item[2]), (activations, projection, section_gain))
    last_out = block_out[-1]
    pooled = lax.optimization_barrier(jnp.mean(last_out.astype(jnp.float32), axis=1))
    pooled_std, pooled_inv = norm_rows(pooled)
    pooled_norm = (pooled_std * final_gain).astype(jnp.bfloat16)
    embedding = jnp.dot(pooled_norm, head_weight, preferred_element_type=jnp.float32)
    image_unit, image_inv = unit_rows(embedding)
    text_unit, text_inv = unit_rows(text_embed.astype(jnp.float32))
    logits = logit_scale * jnp.dot(image_unit, text_unit.T, precision=lax.Precision.HIGHEST)
    count = logits.shape[0]
    targets = (labels[:, None] == jnp.arange(count, dtype=jnp.int32)[None, :]).astype(jnp.float32)
    row_lse = jax.nn.logsumexp(logits, axis=1)
    col_lse = jax.nn.logsumexp(logits, axis=0)
    picked = lax.optimization_barrier(jnp.sum(logits * targets, axis=1))
    col_picked = lax.optimization_barrier(jnp.sum(col_lse[None, :] * targets, axis=1))
    loss_value = 0.5 * jnp.mean(row_lse - picked) + 0.5 * jnp.mean(col_picked - picked)
    section_count = activations.shape[0]
    mean_loss = jnp.zeros((section_count,), jnp.float32).at[-1].set(loss_value)
    row_prob = jnp.exp(logits - row_lse[:, None])
    col_prob = jnp.exp(logits - col_lse[None, :])
    d_logits = 0.5 * (row_prob - targets + (col_prob - targets))
    d_image = logit_scale * jnp.dot(d_logits, text_unit, precision=lax.Precision.HIGHEST)
    d_embedding = (d_image - image_unit * lax.optimization_barrier(jnp.sum(d_image * image_unit, axis=-1, keepdims=True))) * image_inv
    d_pooled_norm = lax.dot_general(d_embedding.astype(jnp.bfloat16), head_weight, (((1,), (1,)), ((), ())), preferred_element_type=jnp.float32)
    d_std = d_pooled_norm * final_gain
    d_pooled = pooled_inv * (d_std - lax.optimization_barrier(jnp.mean(d_std, axis=-1, keepdims=True)) - pooled_std * lax.optimization_barrier(jnp.mean(d_std * pooled_std, axis=-1, keepdims=True)))
    loss_grad = jnp.broadcast_to((d_pooled / TOK)[:, None, :], last_out.shape).astype(jnp.bfloat16)
    d_input = lax.map(lambda item: backward_block(item[0], item[1], item[2], item[3]), (cotangents, saved, projection, section_gain))
    next_act = jnp.concatenate([jnp.zeros_like(block_out[:1]), block_out[:-1]], axis=0)
    next_grad = jnp.concatenate([d_input[1:], loss_grad[None]], axis=0)
    return (next_act, next_grad, mean_loss)
```

```python
import functools
import math

import jax
import jax.numpy as jnp
from jax import lax
from jax.experimental import pallas as pl
from jax.experimental.pallas import tpu as pltpu
from jax.sharding import PartitionSpec as P

epsilon = 1e-06
logit_scale = 100.0
MESH = pl.DeviceIdType.MESH
forward_share = 0.56
backward_share = 0.5


def row_stats(values):
    width = values.shape[-1]
    centre = jnp.sum(values, axis=-1, keepdims=True) / width
    centred = values - centre
    variance = jnp.sum(centred * centred, axis=-1, keepdims=True) / width
    return centre, lax.rsqrt(variance + epsilon)


def step_kernel(
    sections,
    replicas,
    group,
    unit,
    act_ref,
    saved_ref,
    cot_ref,
    weight_ref,
    head_ref,
    scale_ref,
    gain_ref,
    text_ref,
    label_ref,
    next_ref,
    grad_ref,
    loss_ref,
    act,
    saved,
    cot,
    weight,
    normed,
    block,
    d_input,
    slope,
    sum_slope,
    sum_product,
    pooled,
    scale,
    gain,
    text,
    label,
    heads,
    feats,
    columns,
    images,
    texts,
    d_rows,
    part_out,
    part_in,
    relay,
    load_sem,
    weight_sem,
    head_sem,
    bulk_send,
    bulk_recv,
    relay_recv,
    small_send,
    small_recv,
):
    section, replica = lax.axis_index("section"), lax.axis_index("dp")
    last = sections - 1
    tokens, width = act.shape
    rows, span = head_ref.shape
    shards = width // unit
    pairs = (shards - 1) // 2
    slot = lax.rem(replica, group)
    first = replica - slot
    shard = span // group
    f32, bf16 = jnp.float32, jnp.bfloat16
    wide = 2 * unit
    lead = [(0, unit)]
    tail = [(unit + pairs * wide, width - unit - pairs * wide)] if (shards - 1) % 2 else []
    n_chunks = 1 + pairs + len(tail)

    def cut(start, size):
        return pl.ds(start if isinstance(start, int) else pl.multiple_of(start, unit), size)

    def each_chunk(step):
        step(0, 0, unit)
        if pairs:

            def go(index, carry):
                step(index + 1, unit + index * wide, wide)
                return carry

            lax.fori_loop(0, pairs, go, 0)
        for start, size in tail:
            step(n_chunks - 1, start, size)

    static_chunks = (
        lead + [(unit + index * wide, wide) for index in range(pairs)] + tail
    )

    def column_load(index, start, size):
        part = cut(start, size)
        return pltpu.make_async_copy(
            weight_ref.at[:, part], weight.at[:, part], weight_sem.at[index]
        )

    def row_load(index, start, size):
        part = cut(start, size)
        return pltpu.make_async_copy(
            weight_ref.at[part, :], weight.at[part, :], weight_sem.at[index]
        )

    load_act = pltpu.make_async_copy(act_ref, act, load_sem.at[0])
    load_saved = pltpu.make_async_copy(saved_ref, saved, load_sem.at[1])
    load_cot = pltpu.make_async_copy(cot_ref, cot, load_sem.at[2])
    load_scale = pltpu.make_async_copy(scale_ref, scale, load_sem.at[3])
    load_gain = pltpu.make_async_copy(gain_ref, gain, load_sem.at[4])
    load_text = pltpu.make_async_copy(text_ref, text, load_sem.at[5])
    load_label = pltpu.make_async_copy(label_ref, label, load_sem.at[6])

    barrier = pltpu.get_barrier_semaphore()

    def greet(axis, me, peers):
        def go(step, carry):
            peer = lax.rem(me + step, peers)
            pl.semaphore_signal(barrier, inc=1, device_id={axis: peer}, device_id_type=MESH)
            return carry

        lax.fori_loop(1, peers, go, 0)

    greet("section", section, sections)
    load_scale.start()

    @pl.when(section < last)
    def _():
        load_act.start()
        for index, (start, size) in enumerate(static_chunks):
            column_load(index, start, size).start()

        @pl.when(section > 0)
        def _():
            load_saved.start()
            load_cot.start()

    @pl.when(section == last)
    def _():
        greet("dp", replica, replicas)
        load_cot.start()
        for index, (start, size) in enumerate(static_chunks):
            row_load(index, start, size).start()
            if index == 0:
                load_saved.start()
        load_act.start()
        load_text.start()
        load_label.start()
        load_gain.start()

    my_columns = pl.ds(pl.multiple_of(slot * shard, shard), shard)
    away = pl.ds(0, last * rows)

    def head_copy():
        return pltpu.make_async_remote_copy(
            head_ref.at[:, my_columns],
            heads.at[pl.ds(pl.multiple_of(section * rows, rows), rows), :],
            head_sem.at[0],
            head_sem.at[1],
            {"section": last},
            MESH,
        )

    head_arrival = pltpu.make_async_remote_copy(
        heads.at[away, :], heads.at[away, :], head_sem.at[0], head_sem.at[1], {"section": 0}, MESH
    )
    own_head = pltpu.make_async_copy(
        head_ref.at[:, my_columns], heads.at[pl.ds(last * rows, rows), :], head_sem.at[0]
    )

    everything = (slice(None), slice(None))
    forward_send, backward_send, pass_send = bulk_send.at[0], bulk_send.at[1], bulk_send.at[2]
    forward_recv, backward_recv = bulk_recv.at[0], bulk_recv.at[1]

    def move(source, target, send, recv, peer, part):
        return pltpu.make_async_remote_copy(
            source.at[part], target.at[part], send, recv, {"section": peer}, MESH
        )

    def forward_copy(part):
        return move(block, next_ref, forward_send, forward_recv, section + 1, part)

    def backward_copy(part):
        return move(d_input, grad_ref, backward_send, backward_recv, section - 1, part)

    middle = sections // 2
    relays = sections >= 4
    forward_relay, backward_relay = middle + 1, middle - 2

    def rows_at(share):
        edge = int(tokens * share) // 16 * 16
        return pl.ds(0, edge), pl.ds(edge, tokens - edge)

    forward_near, forward_far = rows_at(forward_share)
    backward_near, backward_far = rows_at(backward_share)

    def forward_detour(index, columns_part):
        return move(
            block,
            relay,
            forward_send,
            relay_recv.at[index],
            forward_relay,
            (forward_far, columns_part),
        )

    def backward_detour(index, columns_part):
        return move(
            d_input,
            relay,
            backward_send,
            relay_recv.at[index],
            backward_relay,
            (backward_far, columns_part),
        )

    def forward_pass(columns_part):
        return move(
            relay, next_ref, pass_send, forward_recv, middle, (forward_far, columns_part)
        )

    def backward_pass(columns_part):
        return move(
            relay, grad_ref, pass_send, backward_recv, middle - 1, (backward_far, columns_part)
        )

    def send_piece(direct, detour, origin, near, index, columns_part):
        if not relays:
            direct((slice(None), columns_part)).start()
            return

        @pl.when(section == origin)
        def _():
            direct((near, columns_part)).start()
            detour(index, columns_part).start()

        @pl.when(section != origin)
        def _():
            direct((slice(None), columns_part)).start()

    def forward():
        load_act.wait()
        values = act[...].astype(f32)
        centre, inverse = row_stats(values)
        normed[...] = ((values - centre) * inverse * scale[...]).astype(bf16)

        def step(index, start, size):
            part = cut(start, size)

            @pl.when(section < last)
            def _():
                column_load(index, start, size).wait()

            mixed = jnp.dot(normed[...], weight[:, part], preferred_element_type=f32)
            piece = (act[:, part].astype(f32) + mixed).astype(bf16)
            block[:, part] = piece
            pooled[:, part] = jnp.sum(piece.astype(f32), axis=0, keepdims=True) / tokens

            @pl.when(section < last)
            def _():
                send_piece(forward_copy, forward_detour, middle - 1, forward_near, index, part)

        each_chunk(step)

    def folded(values):
        total = values[:, 0:128]
        for start in range(128, values.shape[-1], 128):
            total = total + values[:, start : start + 128]
        return total

    def backward(wait_rows, before_send):
        load_saved.wait()
        centre, inverse = row_stats(saved[...].astype(f32))
        load_cot.wait()
        sum_slope[...] = jnp.zeros_like(sum_slope)
        sum_product[...] = jnp.zeros_like(sum_product)

        def step(index, start, size):
            part = cut(start, size)
            if wait_rows:
                row_load(index, start, size).wait()
            d_normed = lax.dot_general(
                cot[...],
                weight[part, :],
                (((1,), (1,)), ((), ())),
                preferred_element_type=f32,
            )
            piece = d_normed * scale[:, part]
            slope[:, part] = piece
            sum_slope[...] += folded(piece)
            sum_product[...] += folded(piece * (saved[:, part].astype(f32) - centre))

        each_chunk(step)
        mean_slope = jnp.sum(sum_slope[...], axis=-1, keepdims=True) / width
        mean_product = inverse * (jnp.sum(sum_product[...], axis=-1, keepdims=True) / width)
        offset = inverse * mean_slope
        factor = inverse * inverse * mean_product
        before_send()

        def emit(index, carry):
            part = cut(index * unit, unit)
            d_input[:, part] = (
                cot[:, part].astype(f32)
                + (
                    (inverse * slope[:, part] - offset)
                    - (saved[:, part].astype(f32) - centre) * factor
                )
            ).astype(bf16)
            send_piece(backward_copy, backward_detour, middle, backward_near, index, part)
            return carry

        lax.fori_loop(0, shards, emit, 0)

    def exchange(slots, pair, axis, me, base, peers):
        def go(step, carry):
            peer = lax.rem(me + step, peers)
            pltpu.make_async_remote_copy(
                slots.at[me],
                slots.at[me],
                small_send.at[pair],
                small_recv.at[pair],
                {axis: base + peer},
                MESH,
            ).start()
            return carry

        lax.fori_loop(1, peers, go, 0)

    def settle(slots, pair, peers):
        others = slots.at[pl.ds(0, peers - 1)]
        return pltpu.make_async_remote_copy(
            others, others, small_send.at[pair], small_recv.at[pair], {"dp": 0}, MESH
        )

    @pl.when(section == last)
    def _():
        load_scale.wait()

        def before_send():
            pl.semaphore_wait(barrier, sections + replicas - 2)
            own_head.start()
            load_text.wait()
            load_label.wait()
            values = text[...].astype(f32)
            text_inv = lax.rsqrt(jnp.sum(values * values, axis=-1, keepdims=True) + epsilon)
            texts[replica, :, 0:span] = values * text_inv
            texts[replica, :, span:] = jnp.full((1, 128), label[0]).astype(f32)
            exchange(texts, 0, "dp", replica, 0, replicas)

        backward(True, before_send)

    @pl.when(section < last)
    def _():
        pl.semaphore_wait(barrier, sections - 1)
        head_copy().start()
        load_scale.wait()

    forward()

    @pl.when((section > 0) & (section < last))
    def _():
        backward(False, lambda: None)

    @pl.when(section == 0)
    def _():
        next_ref[...] = jnp.zeros_like(next_ref)

    @pl.when(section < last)
    def _():
        loss_ref[0] = jnp.float32(0)

    def forward_relays():
        def go(index, start, size):
            part = cut(start, size)
            forward_detour(index, part).wait_recv()
            forward_pass(part).start()

        each_chunk(go)

    def backward_relays():
        def go(index, carry):
            part = cut(index * unit, unit)
            backward_detour(index, part).wait_recv()
            backward_pass(part).start()
            return carry

        lax.fori_loop(0, shards, go, 0)

    if relays:

        @pl.when(section == backward_relay)
        def _():
            backward_relays()

        if forward_relay != last:

            @pl.when(section == forward_relay)
            def _():
                forward_relays()

    @pl.when(section == last)
    def _():
        load_gain.wait()
        final_gain = gain[...].reshape(1, width)
        mean_row = pooled[...]
        centre, pooled_inv = row_stats(mean_row)
        pooled_std = (mean_row - centre) * pooled_inv
        feats[slot] = (pooled_std * final_gain).astype(bf16).astype(f32)
        if group > 1:
            exchange(feats, 1, "dp", slot, first, group)
        own_head.wait()
        head_arrival.wait_recv()
        if group > 1:
            settle(feats, 1, group).wait_recv()
        columns[slot] = jnp.dot(
            feats[:, 0, :].astype(bf16), heads[...], preferred_element_type=f32
        )
        if group > 1:
            exchange(columns, 2, "dp", slot, first, group)
        settle(texts, 0, replicas).wait_recv()
        all_text = texts[:, 0, 0:span]
        label_column = texts[:, 0, span : span + 1]
        column = lax.broadcasted_iota(jnp.int32, (replicas, replicas), 1)
        targets = jnp.where(label_column == column.astype(f32), 1.0, 0.0)
        if group > 1:
            settle(columns, 2, group).wait_recv()
        if relays and forward_relay == last:
            forward_relays()
        embedding = jnp.concatenate([columns[index] for index in range(group)], axis=1)
        image_inv = lax.rsqrt(jnp.sum(embedding * embedding, axis=-1, keepdims=True) + epsilon)
        image_unit = embedding * image_inv
        member = lax.broadcasted_iota(jnp.int32, (group, 1), 0)
        if replicas == group:
            all_image = image_unit
        else:
            images[replica] = jnp.sum(
                jnp.where(member == slot, image_unit, 0.0), axis=0, keepdims=True
            )
            exchange(images, 3, "dp", replica, 0, replicas)
            settle(images, 3, replicas).wait_recv()
            all_image = images[:, 0, :]
        logits = logit_scale * lax.dot_general(
            all_image,
            all_text,
            (((1,), (1,)), ((), ())),
            precision=lax.Precision.HIGHEST,
            preferred_element_type=f32,
        )
        row_max = jnp.max(logits, axis=1, keepdims=True)
        row_lse = row_max + jnp.log(jnp.sum(jnp.exp(logits - row_max), axis=1, keepdims=True))
        col_max = jnp.max(logits, axis=0, keepdims=True)
        col_lse = col_max + jnp.log(jnp.sum(jnp.exp(logits - col_max), axis=0, keepdims=True))
        d_logits = 0.5 * (
            (jnp.exp(logits - row_lse) - targets) + (jnp.exp(logits - col_lse) - targets)
        )
        if replicas != group:
            pick_row = lax.broadcasted_iota(jnp.int32, (group, replicas), 0) + first
            pick_column = lax.broadcasted_iota(jnp.int32, (group, replicas), 1)
            d_logits = jnp.dot(
                jnp.where(pick_row == pick_column, 1.0, 0.0),
                d_logits,
                precision=lax.Precision.HIGHEST,
                preferred_element_type=f32,
            )
        d_image = logit_scale * jnp.dot(
            d_logits, all_text, precision=lax.Precision.HIGHEST, preferred_element_type=f32
        )
        along = jnp.sum(d_image * image_unit, axis=-1, keepdims=True)
        d_rows[...] = (d_image - image_unit * along) * image_inv
        partial = lax.dot_general(
            d_rows[:, my_columns].astype(bf16),
            heads[...],
            (((1,), (1,)), ((), ())),
            preferred_element_type=f32,
        )
        for index in range(group):
            part_out[index] = partial[index : index + 1, :]

        def send_part(step, carry):
            peer = lax.rem(slot + step, group)
            pltpu.make_async_remote_copy(
                part_out.at[peer],
                part_in.at[slot],
                small_send.at[4],
                small_recv.at[4],
                {"dp": first + peer},
                MESH,
            ).start()
            return carry

        lax.fori_loop(1, group, send_part, 0)
        part_in[slot] = jnp.sum(jnp.where(member == slot, partial, 0.0), axis=0, keepdims=True)
        picked = jnp.sum(logits * targets, axis=1, keepdims=True)
        col_picked = jnp.sum(col_lse * targets, axis=1, keepdims=True)
        loss = 0.5 * (row_lse - picked) + 0.5 * (col_picked - picked)
        loss_ref[0] = jnp.sum(loss) / replicas
        if group > 1:
            settle(part_in, 4, group).wait_recv()
        d_std = jnp.sum(part_in[...], axis=0) * final_gain
        d_pooled = pooled_inv * (
            d_std
            - jnp.sum(d_std, axis=-1, keepdims=True) / width
            - pooled_std * (jnp.sum(d_std * pooled_std, axis=-1, keepdims=True) / width)
        )
        grad_ref[...] = jnp.broadcast_to(d_pooled / tokens, (tokens, width)).astype(bf16)
        settle(texts, 0, replicas).wait_send()
        if group > 1:
            settle(feats, 1, group).wait_send()
            settle(columns, 2, group).wait_send()
            settle(part_out, 4, group).wait_send()
        if replicas != group:
            settle(images, 3, replicas).wait_send()

    @pl.when(section < last)
    def _():
        head_copy().wait_send()
        forward_copy(everything).wait_send()
        backward_copy(everything).wait_recv()

    @pl.when(section > 0)
    def _():
        backward_copy(everything).wait_send()
        forward_copy(everything).wait_recv()

    if relays:

        @pl.when(section == forward_relay)
        def _():
            forward_pass(slice(None)).wait_send()

        @pl.when(section == backward_relay)
        def _():
            backward_pass(slice(None)).wait_send()


def local(
    activations,
    saved,
    cotangents,
    projection,
    section_gain,
    final_gain,
    head_weight,
    text_embed,
    labels,
):
    sections, replicas = lax.axis_size("section"), lax.axis_size("dp")
    tokens, width = activations.shape[2:]
    rows, span = head_weight.shape
    group = math.gcd(replicas, span // 128)
    shard = span // group
    unit = 256 if width % 256 == 0 else 128
    shards = width // unit
    chunks = 1 + (shards - 1) // 2 + (shards - 1) % 2
    f32, bf16 = jnp.float32, jnp.bfloat16
    dma = pltpu.SemaphoreType.DMA
    vmem = pl.BlockSpec(memory_space=pltpu.VMEM)
    whole = pl.BlockSpec(memory_space=pl.ANY)
    big = pltpu.VMEM((tokens, width), bf16)
    next_raw, grad_raw, loss = pl.pallas_call(
        functools.partial(step_kernel, sections, replicas, group, unit),
        out_shape=(big, big, jax.ShapeDtypeStruct((1,), f32)),
        in_specs=[whole] * 9,
        out_specs=(vmem, vmem, pl.BlockSpec(memory_space=pltpu.SMEM)),
        scratch_shapes=[
            big,
            big,
            big,
            pltpu.VMEM((width, width), bf16),
            big,
            big,
            big,
            pltpu.VMEM((tokens, width), f32),
            pltpu.VMEM((tokens, 128), f32),
            pltpu.VMEM((tokens, 128), f32),
            pltpu.VMEM((1, width), f32),
            pltpu.VMEM((1, width), f32),
            pltpu.VMEM((width,), f32),
            pltpu.VMEM((1, span), bf16),
            pltpu.SMEM((1,), jnp.int32),
            pltpu.VMEM((sections * rows, shard), bf16),
            pltpu.VMEM((group, 1, width), f32),
            pltpu.VMEM((group, group, shard), f32),
            pltpu.VMEM((replicas, 1, span), f32),
            pltpu.VMEM((replicas, 1, span + 128), f32),
            pltpu.VMEM((group, span), f32),
            pltpu.VMEM((group, 1, width), f32),
            pltpu.VMEM((group, 1, width), f32),
            big,
            dma((7,)),
            dma((chunks,)),
            dma((2,)),
            dma((3,)),
            dma((2,)),
            dma((shards,)),
            dma((5,)),
            dma((5,)),
        ],
        compiler_params=pltpu.CompilerParams(
            collective_id=0, has_side_effects=True, vmem_limit_bytes=40 * 1024 * 1024
        ),
        name="tower_step",
    )(
        activations[0, 0],
        saved[0, 0],
        cotangents[0, 0],
        projection[0],
        head_weight,
        section_gain,
        final_gain,
        text_embed,
        labels,
    )
    return (next_raw[None, None], grad_raw[None, None], loss)


def solution(mesh):
    return jax.shard_map(
        local,
        mesh=mesh,
        in_specs=(
            P("section", "dp", None, None),
            P("section", "dp", None, None),
            P("section", "dp", None, None),
            P("section", None, None),
            P("section", None),
            P(),
            P("section", None),
            P("dp", None),
            P("dp"),
        ),
        out_specs=(P("section", "dp", None, None), P("section", "dp", None, None), P("section")),
        check_vma=False,
    )
```

```python
import functools
import math

import jax
import jax.numpy as jnp
from jax import lax
from jax.experimental import pallas as pl
from jax.experimental.pallas import tpu as pltpu
from jax.sharding import PartitionSpec as P

epsilon = 1e-06
logit_scale = 100.0
MESH = pl.DeviceIdType.MESH
forward_share = 0.56
backward_share = 0.5


def row_stats(values):
    width = values.shape[-1]
    centre = jnp.sum(values, axis=-1, keepdims=True) / width
    centred = values - centre
    variance = jnp.sum(centred * centred, axis=-1, keepdims=True) / width
    return centre, lax.rsqrt(variance + epsilon)


def step_kernel(
    sections,
    replicas,
    group,
    unit,
    act_ref,
    saved_ref,
    cot_ref,
    weight_ref,
    head_ref,
    scale_ref,
    gain_ref,
    text_ref,
    label_ref,
    next_ref,
    grad_ref,
    loss_ref,
    act,
    saved,
    cot,
    weight,
    normed,
    block,
    d_input,
    slope,
    sum_slope,
    sum_product,
    pooled,
    scale,
    gain,
    text,
    heads,
    feats,
    columns,
    images,
    texts,
    d_rows,
    part_out,
    part_in,
    relay,
    load_sem,
    weight_sem,
    head_sem,
    bulk_send,
    bulk_recv,
    relay_recv,
    small_send,
    small_recv,
):
    section, replica = lax.axis_index("section"), lax.axis_index("dp")
    last = sections - 1
    tokens, width = act.shape
    rows, span = head_ref.shape
    shards = width // unit
    pairs = (shards - 1) // 2
    slot = lax.rem(replica, group)
    first = replica - slot
    shard = span // group
    f32, bf16 = jnp.float32, jnp.bfloat16
    wide = 2 * unit
    lead = [(0, unit)]
    tail = [(unit + pairs * wide, width - unit - pairs * wide)] if (shards - 1) % 2 else []
    n_chunks = 1 + pairs + len(tail)

    def cut(start, size):
        return pl.ds(start if isinstance(start, int) else pl.multiple_of(start, unit), size)

    def each_chunk(step):
        step(0, 0, unit)
        if pairs:

            def go(index, carry):
                step(index + 1, unit + index * wide, wide)
                return carry

            lax.fori_loop(0, pairs, go, 0)
        for start, size in tail:
            step(n_chunks - 1, start, size)

    static_chunks = (
        lead + [(unit + index * wide, wide) for index in range(pairs)] + tail
    )

    def column_load(index, start, size):
        part = cut(start, size)
        return pltpu.make_async_copy(
            weight_ref.at[:, part], weight.at[:, part], weight_sem.at[index]
        )

    def row_load(index, start, size):
        part = cut(start, size)
        return pltpu.make_async_copy(
            weight_ref.at[part, :], weight.at[part, :], weight_sem.at[index]
        )

    load_act = pltpu.make_async_copy(act_ref, act, load_sem.at[0])
    load_saved = pltpu.make_async_copy(saved_ref, saved, load_sem.at[1])
    load_cot = pltpu.make_async_copy(cot_ref, cot, load_sem.at[2])
    load_scale = pltpu.make_async_copy(scale_ref, scale, load_sem.at[3])
    load_gain = pltpu.make_async_copy(gain_ref, gain, load_sem.at[4])
    load_text = pltpu.make_async_copy(text_ref, text, load_sem.at[5])

    barrier = pltpu.get_barrier_semaphore()

    def greet(axis, me, peers):
        def go(step, carry):
            peer = lax.rem(me + step, peers)
            pl.semaphore_signal(barrier, inc=1, device_id={axis: peer}, device_id_type=MESH)
            return carry

        lax.fori_loop(1, peers, go, 0)

    greet("section", section, sections)
    load_scale.start()

    @pl.when(section < last)
    def _():
        load_act.start()
        for index, (start, size) in enumerate(static_chunks):
            column_load(index, start, size).start()

        @pl.when(section > 0)
        def _():
            load_saved.start()
            load_cot.start()

    @pl.when(section == last)
    def _():
        greet("dp", replica, replicas)
        load_cot.start()
        for index, (start, size) in enumerate(static_chunks):
            row_load(index, start, size).start()
            if index == 0:
                load_saved.start()
        load_act.start()
        load_text.start()
        load_gain.start()

    my_columns = pl.ds(pl.multiple_of(slot * shard, shard), shard)
    away = pl.ds(0, last * rows)

    def head_copy():
        return pltpu.make_async_remote_copy(
            head_ref.at[:, my_columns],
            heads.at[pl.ds(pl.multiple_of(section * rows, rows), rows), :],
            head_sem.at[0],
            head_sem.at[1],
            {"section": last},
            MESH,
        )

    head_arrival = pltpu.make_async_remote_copy(
        heads.at[away, :], heads.at[away, :], head_sem.at[0], head_sem.at[1], {"section": 0}, MESH
    )
    own_head = pltpu.make_async_copy(
        head_ref.at[:, my_columns], heads.at[pl.ds(last * rows, rows), :], head_sem.at[0]
    )

    everything = (slice(None), slice(None))
    forward_send, backward_send, pass_send = bulk_send.at[0], bulk_send.at[1], bulk_send.at[2]
    forward_recv, backward_recv = bulk_recv.at[0], bulk_recv.at[1]

    def move(source, target, send, recv, peer, part):
        return pltpu.make_async_remote_copy(
            source.at[part], target.at[part], send, recv, {"section": peer}, MESH
        )

    def forward_copy(part):
        return move(block, next_ref, forward_send, forward_recv, section + 1, part)

    def backward_copy(part):
        return move(d_input, grad_ref, backward_send, backward_recv, section - 1, part)

    middle = sections // 2
    relays = sections >= 4
    forward_relay, backward_relay = middle + 1, middle - 2

    def rows_at(share):
        edge = int(tokens * share) // 16 * 16
        return pl.ds(0, edge), pl.ds(edge, tokens - edge)

    forward_near, forward_far = rows_at(forward_share)
    backward_near, backward_far = rows_at(backward_share)

    def forward_detour(index, columns_part):
        return move(
            block,
            relay,
            forward_send,
            relay_recv.at[index],
            forward_relay,
            (forward_far, columns_part),
        )

    def backward_detour(index, columns_part):
        return move(
            d_input,
            relay,
            backward_send,
            relay_recv.at[index],
            backward_relay,
            (backward_far, columns_part),
        )

    def forward_pass(columns_part):
        return move(
            relay, next_ref, pass_send, forward_recv, middle, (forward_far, columns_part)
        )

    def backward_pass(columns_part):
        return move(
            relay, grad_ref, pass_send, backward_recv, middle - 1, (backward_far, columns_part)
        )

    def send_piece(direct, detour, origin, near, index, columns_part):
        if not relays:
            direct((slice(None), columns_part)).start()
            return

        @pl.when(section == origin)
        def _():
            direct((near, columns_part)).start()
            detour(index, columns_part).start()

        @pl.when(section != origin)
        def _():
            direct((slice(None), columns_part)).start()

    def forward():
        load_act.wait()
        values = act[...].astype(f32)
        centre, inverse = row_stats(values)
        normed[...] = ((values - centre) * inverse * scale[...]).astype(bf16)

        def step(index, start, size):
            part = cut(start, size)

            @pl.when(section < last)
            def _():
                column_load(index, start, size).wait()

            mixed = jnp.dot(normed[...], weight[:, part], preferred_element_type=f32)
            piece = (act[:, part].astype(f32) + mixed).astype(bf16)
            block[:, part] = piece
            pooled[:, part] = jnp.sum(piece.astype(f32), axis=0, keepdims=True) / tokens

            @pl.when(section < last)
            def _():
                send_piece(forward_copy, forward_detour, middle - 1, forward_near, index, part)

        each_chunk(step)

    def folded(values):
        total = values[:, 0:128]
        for start in range(128, values.shape[-1], 128):
            total = total + values[:, start : start + 128]
        return total

    def backward(wait_rows, before_send):
        load_saved.wait()
        centre, inverse = row_stats(saved[...].astype(f32))
        load_cot.wait()
        sum_slope[...] = jnp.zeros_like(sum_slope)
        sum_product[...] = jnp.zeros_like(sum_product)

        def step(index, start, size):
            part = cut(start, size)
            if wait_rows:
                row_load(index, start, size).wait()
            d_normed = lax.dot_general(
                cot[...],
                weight[part, :],
                (((1,), (1,)), ((), ())),
                preferred_element_type=f32,
            )
            piece = d_normed * scale[:, part]
            slope[:, part] = piece
            sum_slope[...] += folded(piece)
            sum_product[...] += folded(piece * (saved[:, part].astype(f32) - centre))

        each_chunk(step)
        mean_slope = jnp.sum(sum_slope[...], axis=-1, keepdims=True) / width
        mean_product = inverse * (jnp.sum(sum_product[...], axis=-1, keepdims=True) / width)
        offset = inverse * mean_slope
        factor = inverse * inverse * mean_product
        before_send()

        def emit(index, carry):
            part = cut(index * unit, unit)
            d_input[:, part] = (
                cot[:, part].astype(f32)
                + (
                    (inverse * slope[:, part] - offset)
                    - (saved[:, part].astype(f32) - centre) * factor
                )
            ).astype(bf16)
            send_piece(backward_copy, backward_detour, middle, backward_near, index, part)
            return carry

        lax.fori_loop(0, shards, emit, 0)

    def exchange(slots, pair, axis, me, base, peers):
        def go(step, carry):
            peer = lax.rem(me + step, peers)
            pltpu.make_async_remote_copy(
                slots.at[me],
                slots.at[me],
                small_send.at[pair],
                small_recv.at[pair],
                {axis: base + peer},
                MESH,
            ).start()
            return carry

        lax.fori_loop(1, peers, go, 0)

    def settle(slots, pair, peers):
        others = slots.at[pl.ds(0, peers - 1)]
        return pltpu.make_async_remote_copy(
            others, others, small_send.at[pair], small_recv.at[pair], {"dp": 0}, MESH
        )

    @pl.when(section == last)
    def _():
        load_scale.wait()

        def before_send():
            pl.semaphore_wait(barrier, sections + replicas - 2)
            own_head.start()
            load_text.wait()
            values = text[...].astype(f32)
            text_inv = lax.rsqrt(jnp.sum(values * values, axis=-1, keepdims=True) + epsilon)
            texts[replica, :, 0:span] = values * text_inv
            texts[replica, :, span:] = jnp.full((1, 128), label_ref[0]).astype(f32)
            exchange(texts, 0, "dp", replica, 0, replicas)

        backward(True, before_send)

    @pl.when(section < last)
    def _():
        pl.semaphore_wait(barrier, sections - 1)
        head_copy().start()
        load_scale.wait()

    forward()

    @pl.when((section > 0) & (section < last))
    def _():
        backward(False, lambda: None)

    @pl.when(section == 0)
    def _():
        next_ref[...] = jnp.zeros_like(next_ref)

    @pl.when(section < last)
    def _():
        loss_ref[...] = jnp.zeros_like(loss_ref)

    def forward_relays():
        def go(index, start, size):
            part = cut(start, size)
            forward_detour(index, part).wait_recv()
            forward_pass(part).start()

        each_chunk(go)

    def backward_relays():
        def go(index, carry):
            part = cut(index * unit, unit)
            backward_detour(index, part).wait_recv()
            backward_pass(part).start()
            return carry

        lax.fori_loop(0, shards, go, 0)

    if relays:

        @pl.when(section == backward_relay)
        def _():
            backward_relays()

        if forward_relay != last:

            @pl.when(section == forward_relay)
            def _():
                forward_relays()

    @pl.when(section == last)
    def _():
        load_gain.wait()
        final_gain = gain[...].reshape(1, width)
        mean_row = pooled[...]
        centre, pooled_inv = row_stats(mean_row)
        pooled_std = (mean_row - centre) * pooled_inv
        feats[slot] = (pooled_std * final_gain).astype(bf16).astype(f32)
        if group > 1:
            exchange(feats, 1, "dp", slot, first, group)
        own_head.wait()
        head_arrival.wait_recv()
        if group > 1:
            settle(feats, 1, group).wait_recv()
        columns[slot] = jnp.dot(
            feats[:, 0, :].astype(bf16), heads[...], preferred_element_type=f32
        )
        if group > 1:
            exchange(columns, 2, "dp", slot, first, group)
        settle(texts, 0, replicas).wait_recv()
        all_text = texts[:, 0, 0:span]
        label_column = texts[:, 0, span : span + 1]
        column = lax.broadcasted_iota(jnp.int32, (replicas, replicas), 1)
        targets = jnp.where(label_column == column.astype(f32), 1.0, 0.0)
        if group > 1:
            settle(columns, 2, group).wait_recv()
        if relays and forward_relay == last:
            forward_relays()
        embedding = jnp.concatenate([columns[index] for index in range(group)], axis=1)
        image_inv = lax.rsqrt(jnp.sum(embedding * embedding, axis=-1, keepdims=True) + epsilon)
        image_unit = embedding * image_inv
        member = lax.broadcasted_iota(jnp.int32, (group, 1), 0)
        if replicas == group:
            all_image = image_unit
        else:
            images[replica] = jnp.sum(
                jnp.where(member == slot, image_unit, 0.0), axis=0, keepdims=True
            )
            exchange(images, 3, "dp", replica, 0, replicas)
            settle(images, 3, replicas).wait_recv()
            all_image = images[:, 0, :]
        logits = logit_scale * lax.dot_general(
            all_image,
            all_text,
            (((1,), (1,)), ((), ())),
            precision=lax.Precision.HIGHEST,
            preferred_element_type=f32,
        )
        row_max = jnp.max(logits, axis=1, keepdims=True)
        row_lse = row_max + jnp.log(jnp.sum(jnp.exp(logits - row_max), axis=1, keepdims=True))
        col_max = jnp.max(logits, axis=0, keepdims=True)
        col_lse = col_max + jnp.log(jnp.sum(jnp.exp(logits - col_max), axis=0, keepdims=True))
        d_logits = 0.5 * (
            (jnp.exp(logits - row_lse) - targets) + (jnp.exp(logits - col_lse) - targets)
        )
        if replicas != group:
            pick_row = lax.broadcasted_iota(jnp.int32, (group, replicas), 0) + first
            pick_column = lax.broadcasted_iota(jnp.int32, (group, replicas), 1)
            d_logits = jnp.dot(
                jnp.where(pick_row == pick_column, 1.0, 0.0),
                d_logits,
                precision=lax.Precision.HIGHEST,
                preferred_element_type=f32,
            )
        d_image = logit_scale * jnp.dot(
            d_logits, all_text, precision=lax.Precision.HIGHEST, preferred_element_type=f32
        )
        along = jnp.sum(d_image * image_unit, axis=-1, keepdims=True)
        d_rows[...] = (d_image - image_unit * along) * image_inv
        partial = lax.dot_general(
            d_rows[:, my_columns].astype(bf16),
            heads[...],
            (((1,), (1,)), ((), ())),
            preferred_element_type=f32,
        )
        for index in range(group):
            part_out[index] = partial[index : index + 1, :]

        def send_part(step, carry):
            peer = lax.rem(slot + step, group)
            pltpu.make_async_remote_copy(
                part_out.at[peer],
                part_in.at[slot],
                small_send.at[4],
                small_recv.at[4],
                {"dp": first + peer},
                MESH,
            ).start()
            return carry

        lax.fori_loop(1, group, send_part, 0)
        part_in[slot] = jnp.sum(jnp.where(member == slot, partial, 0.0), axis=0, keepdims=True)
        picked = jnp.sum(logits * targets, axis=1, keepdims=True)
        col_picked = jnp.sum(col_lse * targets, axis=1, keepdims=True)
        loss = 0.5 * (row_lse - picked) + 0.5 * (col_picked - picked)
        loss_ref[...] = jnp.broadcast_to(
            jnp.sum(loss, axis=0, keepdims=True) / replicas, loss_ref.shape
        )
        if group > 1:
            settle(part_in, 4, group).wait_recv()
        d_std = jnp.sum(part_in[...], axis=0) * final_gain
        d_pooled = pooled_inv * (
            d_std
            - jnp.sum(d_std, axis=-1, keepdims=True) / width
            - pooled_std * (jnp.sum(d_std * pooled_std, axis=-1, keepdims=True) / width)
        )
        grad_ref[...] = jnp.broadcast_to(d_pooled / tokens, (tokens, width)).astype(bf16)
        settle(texts, 0, replicas).wait_send()
        if group > 1:
            settle(feats, 1, group).wait_send()
            settle(columns, 2, group).wait_send()
            settle(part_out, 4, group).wait_send()
        if replicas != group:
            settle(images, 3, replicas).wait_send()

    @pl.when(section < last)
    def _():
        head_copy().wait_send()
        forward_copy(everything).wait_send()
        backward_copy(everything).wait_recv()

    @pl.when(section > 0)
    def _():
        backward_copy(everything).wait_send()
        forward_copy(everything).wait_recv()

    if relays:

        @pl.when(section == forward_relay)
        def _():
            forward_pass(slice(None)).wait_send()

        @pl.when(section == backward_relay)
        def _():
            backward_pass(slice(None)).wait_send()


def deliver(next_ref, grad_ref, loss_ref, next_out, grad_out, loss_out, sem):
    copies = [
        pltpu.make_async_copy(source, target, sem.at[index])
        for index, (source, target) in enumerate(
            ((next_ref, next_out), (grad_ref, grad_out), (loss_ref, loss_out))
        )
    ]
    for copy in copies:
        copy.start()
    for copy in copies:
        copy.wait()


def in_hbm(value):
    return pltpu.with_memory_space_constraint(value, pltpu.HBM)


def local(
    activations,
    saved,
    cotangents,
    projection,
    section_gain,
    final_gain,
    head_weight,
    text_embed,
    labels,
):
    sections, replicas = lax.axis_size("section"), lax.axis_size("dp")
    tokens, width = activations.shape[2:]
    rows, span = head_weight.shape
    group = math.gcd(replicas, span // 128)
    shard = span // group
    unit = 256 if width % 256 == 0 else 128
    shards = width // unit
    chunks = 1 + (shards - 1) // 2 + (shards - 1) % 2
    f32, bf16 = jnp.float32, jnp.bfloat16
    dma = pltpu.SemaphoreType.DMA
    vmem = pl.BlockSpec(memory_space=pltpu.VMEM)
    hbm = pl.BlockSpec(memory_space=pltpu.HBM)
    big = pltpu.VMEM((tokens, width), bf16)
    next_raw, grad_raw, loss = pl.pallas_call(
        functools.partial(step_kernel, sections, replicas, group, unit),
        out_shape=(big, big, pltpu.VMEM((1, 128), f32)),
        in_specs=[hbm] * 8 + [pl.BlockSpec(memory_space=pltpu.SMEM)],
        out_specs=(vmem, vmem, vmem),
        scratch_shapes=[
            big,
            big,
            big,
            pltpu.VMEM((width, width), bf16),
            big,
            big,
            big,
            pltpu.VMEM((tokens, width), f32),
            pltpu.VMEM((tokens, 128), f32),
            pltpu.VMEM((tokens, 128), f32),
            pltpu.VMEM((1, width), f32),
            pltpu.VMEM((1, width), f32),
            pltpu.VMEM((width,), f32),
            pltpu.VMEM((1, span), bf16),
            pltpu.VMEM((sections * rows, shard), bf16),
            pltpu.VMEM((group, 1, width), f32),
            pltpu.VMEM((group, group, shard), f32),
            pltpu.VMEM((replicas, 1, span), f32),
            pltpu.VMEM((replicas, 1, span + 128), f32),
            pltpu.VMEM((group, span), f32),
            pltpu.VMEM((group, 1, width), f32),
            pltpu.VMEM((group, 1, width), f32),
            big,
            dma((6,)),
            dma((chunks,)),
            dma((2,)),
            dma((3,)),
            dma((2,)),
            dma((shards,)),
            dma((5,)),
            dma((5,)),
        ],
        compiler_params=pltpu.CompilerParams(
            collective_id=0, has_side_effects=True, vmem_limit_bytes=40 * 1024 * 1024
        ),
        name="tower_step",
    )(
        in_hbm(activations[0, 0]),
        in_hbm(saved[0, 0]),
        in_hbm(cotangents[0, 0]),
        in_hbm(projection[0]),
        in_hbm(head_weight),
        in_hbm(section_gain),
        in_hbm(final_gain),
        in_hbm(text_embed),
        labels,
    )
    out = pltpu.HBM((tokens, width), bf16)
    next_act, next_grad, mean_loss = pl.pallas_call(
        deliver,
        out_shape=(out, out, pltpu.HBM((1, 128), f32)),
        in_specs=[vmem, vmem, vmem],
        out_specs=(hbm, hbm, hbm),
        scratch_shapes=[dma((3,))],
        name="deliver",
    )(
        pltpu.with_memory_space_constraint(next_raw, pltpu.VMEM),
        pltpu.with_memory_space_constraint(grad_raw, pltpu.VMEM),
        pltpu.with_memory_space_constraint(loss, pltpu.VMEM),
    )
    return (next_act[None, None], next_grad[None, None], mean_loss[0, :1])


def solution(mesh):
    return jax.shard_map(
        local,
        mesh=mesh,
        in_specs=(
            P("section", "dp", None, None),
            P("section", "dp", None, None),
            P("section", "dp", None, None),
            P("section", None, None),
            P("section", None),
            P(),
            P("section", None),
            P("dp", None),
            P("dp"),
        ),
        out_specs=(P("section", "dp", None, None), P("section", "dp", None, None), P("section")),
        check_vma=False,
    )
```

```python
import functools
import math

import jax
import jax.numpy as jnp
from jax import lax
from jax.experimental import pallas as pl
from jax.experimental.pallas import tpu as pltpu
from jax.sharding import PartitionSpec as P

epsilon = 1e-06
logit_scale = 100.0
MESH = pl.DeviceIdType.MESH
forward_share = 0.58
backward_share = 0.5


def row_stats(values):
    width = values.shape[-1]
    centre = jnp.sum(values, axis=-1, keepdims=True) / width
    centred = values - centre
    variance = jnp.sum(centred * centred, axis=-1, keepdims=True) / width
    return centre, lax.rsqrt(variance + epsilon)


def step_kernel(
    sections,
    replicas,
    group,
    unit,
    act_ref,
    saved_ref,
    cot_ref,
    weight_ref,
    head_ref,
    scale_ref,
    gain_ref,
    text_ref,
    label_ref,
    next_ref,
    grad_ref,
    loss_ref,
    act,
    saved,
    cot,
    weight,
    normed,
    block,
    d_input,
    slope,
    sum_slope,
    sum_product,
    pooled,
    scale,
    gain,
    text,
    heads,
    feats,
    columns,
    images,
    texts,
    d_rows,
    part_out,
    part_in,
    relay,
    load_sem,
    weight_sem,
    head_sem,
    bulk_send,
    bulk_recv,
    relay_recv,
    small_send,
    small_recv,
    ready,
):
    section, replica = lax.axis_index("section"), lax.axis_index("dp")
    last = sections - 1
    tokens, width = act.shape
    rows, span = head_ref.shape
    shards = width // unit
    pairs = (shards - 1) // 2
    slot = lax.rem(replica, group)
    first = replica - slot
    shard = span // group
    f32, bf16 = jnp.float32, jnp.bfloat16
    wide = 2 * unit
    lead = [(0, unit)]
    tail = [(unit + pairs * wide, width - unit - pairs * wide)] if (shards - 1) % 2 else []
    n_chunks = 1 + pairs + len(tail)

    def cut(start, size):
        return pl.ds(start if isinstance(start, int) else pl.multiple_of(start, unit), size)

    def each_chunk(step):
        step(0, 0, unit)
        if pairs:

            def go(index, carry):
                step(index + 1, unit + index * wide, wide)
                return carry

            lax.fori_loop(0, pairs, go, 0)
        for start, size in tail:
            step(n_chunks - 1, start, size)

    static_chunks = (
        lead + [(unit + index * wide, wide) for index in range(pairs)] + tail
    )

    def column_load(index, start, size):
        part = cut(start, size)
        return pltpu.make_async_copy(
            weight_ref.at[:, part], weight.at[:, part], weight_sem.at[index]
        )

    def row_load(index, start, size):
        part = cut(start, size)
        return pltpu.make_async_copy(
            weight_ref.at[part, :], weight.at[part, :], weight_sem.at[index]
        )

    edge = int(tokens * forward_share) // 16 * 16
    row_parts = (pl.ds(0, edge), pl.ds(edge, tokens - edge))

    def load_act(part):
        picked = row_parts[part]
        return pltpu.make_async_copy(
            act_ref.at[picked, :], act.at[picked, :], load_sem.at[(0, 6)[part]]
        )

    load_saved = pltpu.make_async_copy(saved_ref, saved, load_sem.at[1])
    load_cot = pltpu.make_async_copy(cot_ref, cot, load_sem.at[2])
    load_scale = pltpu.make_async_copy(scale_ref, scale, load_sem.at[3])
    load_gain = pltpu.make_async_copy(gain_ref, gain, load_sem.at[4])
    load_text = pltpu.make_async_copy(text_ref, text, load_sem.at[5])

    barrier = pltpu.get_barrier_semaphore()

    def greet(axis, me, peers, skip):
        def go(step, carry):
            peer = lax.rem(me + step, peers)

            @pl.when(jnp.abs(me - peer) != skip)
            def _():
                pl.semaphore_signal(barrier, inc=1, device_id={axis: peer}, device_id_type=MESH)

            return carry

        lax.fori_loop(1, peers, go, 0)

    @pl.when(section < last)
    def _():
        load_act(0).start()
        load_scale.start()
        column_load(0, *static_chunks[0]).start()
        load_act(1).start()

    def other_loads():
        for index, (start, size) in list(enumerate(static_chunks))[1:]:
            column_load(index, start, size).start()

        @pl.when(section > 0)
        def _():
            load_saved.start()
            load_cot.start()

    @pl.when(section == last)
    def _():
        load_saved.start()
        load_cot.start()
        load_scale.start()
        for index, (start, size) in enumerate(static_chunks):
            row_load(index, start, size).start()
        load_act(0).start()
        load_act(1).start()
        load_text.start()
        load_gain.start()

    direct = sections < 4
    greet("section", section, sections, sections if direct else last)

    @pl.when(section == last)
    def _():
        greet("dp", replica, replicas, replicas)

    my_columns = pl.ds(pl.multiple_of(slot * shard, shard), shard)
    away = pl.ds(0, last * rows)

    def head_copy():
        return pltpu.make_async_remote_copy(
            head_ref.at[:, my_columns],
            heads.at[pl.ds(pl.multiple_of(section * rows, rows), rows), :],
            head_sem.at[0],
            head_sem.at[1],
            {"section": last},
            MESH,
        )

    head_arrival = pltpu.make_async_remote_copy(
        heads.at[away, :], heads.at[away, :], head_sem.at[0], head_sem.at[1], {"section": 0}, MESH
    )
    own_head = pltpu.make_async_copy(
        head_ref.at[:, my_columns], heads.at[pl.ds(last * rows, rows), :], head_sem.at[0]
    )

    everything = (slice(None), slice(None))
    forward_send, backward_send, pass_send = bulk_send.at[0], bulk_send.at[1], bulk_send.at[2]
    forward_recv, backward_recv = bulk_recv.at[0], bulk_recv.at[1]

    def move(source, target, send, recv, peer, part):
        return pltpu.make_async_remote_copy(
            source.at[part], target.at[part], send, recv, {"section": peer}, MESH
        )

    def forward_copy(part):
        return move(block, next_ref, forward_send, forward_recv, section + 1, part)

    def backward_copy(part):
        return move(d_input, grad_ref, backward_send, backward_recv, section - 1, part)

    middle = sections // 2
    relays = sections >= 4
    forward_relay, backward_relay = middle + 1, middle - 2

    forward_near, forward_far = row_parts
    bend = int(tokens * backward_share) // 16 * 16
    backward_near, backward_far = pl.ds(0, bend), pl.ds(bend, tokens - bend)

    def forward_detour(index, columns_part):
        return move(
            block,
            relay,
            forward_send,
            relay_recv.at[index],
            forward_relay,
            (forward_far, columns_part),
        )

    def backward_detour(index, columns_part):
        return move(
            d_input,
            relay,
            backward_send,
            relay_recv.at[index],
            backward_relay,
            (backward_far, columns_part),
        )

    def forward_pass(columns_part):
        return move(
            relay, next_ref, pass_send, forward_recv, middle, (forward_far, columns_part)
        )

    def backward_pass(columns_part):
        return move(
            relay, grad_ref, pass_send, backward_recv, middle - 1, (backward_far, columns_part)
        )

    def send_backward(index, columns_part):
        if not relays:
            backward_copy((slice(None), columns_part)).start()
            return

        @pl.when(section == middle)
        def _():
            backward_copy((backward_near, columns_part)).start()
            backward_detour(index, columns_part).start()

        @pl.when(section != middle)
        def _():
            backward_copy((slice(None), columns_part)).start()

    def send_forward(index, columns_part, part):
        picked = row_parts[part]
        if part == 0 or not relays:
            forward_copy((picked, columns_part)).start()
            return

        @pl.when(section == middle - 1)
        def _():
            forward_detour(index, columns_part).start()

        @pl.when(section != middle - 1)
        def _():
            forward_copy((picked, columns_part)).start()

    def normalise(part):
        picked = row_parts[part]
        load_act(part).wait()
        if part == 0:

            @pl.when(section < last)
            def _():
                other_loads()

        values = act[picked, :].astype(f32)
        centre, inverse = row_stats(values)
        if part == 0:

            @pl.when(section < last)
            def _():
                load_scale.wait()

        normed[picked, :] = ((values - centre) * inverse * scale[...]).astype(bf16)

    def mix(picked, columns_part):
        mixed = jnp.dot(
            normed[picked, :], weight[:, columns_part], preferred_element_type=f32
        )
        piece = (act[picked, columns_part].astype(f32) + mixed).astype(bf16)
        block[picked, columns_part] = piece
        return jnp.sum(piece.astype(f32), axis=0, keepdims=True)

    def forward(before, between):
        narrow = cut(*lead[0])
        total = jnp.zeros((1, unit), f32)
        for part in range(2):
            normalise(part)
            if part == 0:

                @pl.when(section < last)
                def _():
                    column_load(0, *lead[0]).wait()

            total = total + mix(row_parts[part], narrow)
            if part == 0:
                before()

            @pl.when(section < last)
            def _():
                send_forward(0, narrow, part)

        pooled[:, narrow] = total / tokens
        between()

        def step(index, start, size):
            columns_part = cut(start, size)

            @pl.when(section < last)
            def _():
                column_load(index, start, size).wait()

            pooled[:, columns_part] = mix(slice(None), columns_part) / tokens

            @pl.when(section < last)
            def _():
                if relays:
                    for part in range(2):
                        send_forward(index, columns_part, part)
                else:
                    forward_copy((slice(None), columns_part)).start()

        if pairs:

            def go(index, carry):
                step(index + 1, unit + index * wide, wide)
                return carry

            lax.fori_loop(0, pairs, go, 0)
        for start, size in tail:
            step(n_chunks - 1, start, size)

    def folded(values):
        total = values[:, 0:128]
        for start in range(128, values.shape[-1], 128):
            total = total + values[:, start : start + 128]
        return total

    def backward(wait_rows, before_send):
        load_saved.wait()
        centre, inverse = row_stats(saved[...].astype(f32))
        load_cot.wait()
        if wait_rows:
            load_scale.wait()
        sum_slope[...] = jnp.zeros_like(sum_slope)
        sum_product[...] = jnp.zeros_like(sum_product)

        def step(index, start, size):
            part = cut(start, size)
            if wait_rows:
                row_load(index, start, size).wait()
            d_normed = lax.dot_general(
                cot[...],
                weight[part, :],
                (((1,), (1,)), ((), ())),
                preferred_element_type=f32,
            )
            piece = d_normed * scale[:, part]
            slope[:, part] = piece
            sum_slope[...] += folded(piece)
            sum_product[...] += folded(piece * (saved[:, part].astype(f32) - centre))

        each_chunk(step)
        mean_slope = jnp.sum(sum_slope[...], axis=-1, keepdims=True) / width
        mean_product = inverse * (jnp.sum(sum_product[...], axis=-1, keepdims=True) / width)
        offset = inverse * mean_slope
        factor = inverse * inverse * mean_product
        before_send()

        def emit(index, carry):
            part = cut(index * unit, unit)
            d_input[:, part] = (
                cot[:, part].astype(f32)
                + (
                    (inverse * slope[:, part] - offset)
                    - (saved[:, part].astype(f32) - centre) * factor
                )
            ).astype(bf16)
            send_backward(index, part)
            return carry

        lax.fori_loop(0, shards, emit, 0)

    def exchange(slots, pair, axis, me, base, peers):
        def go(step, carry):
            peer = lax.rem(me + step, peers)
            pltpu.make_async_remote_copy(
                slots.at[me],
                slots.at[me],
                small_send.at[pair],
                small_recv.at[pair],
                {axis: base + peer},
                MESH,
            ).start()
            return carry

        lax.fori_loop(1, peers, go, 0)

    def settle(slots, pair, peers):
        others = slots.at[pl.ds(0, peers - 1)]
        return pltpu.make_async_remote_copy(
            others, others, small_send.at[pair], small_recv.at[pair], {"dp": 0}, MESH
        )

    @pl.when(section == last)
    def _():
        def before_send():
            pl.semaphore_wait(barrier, sections + replicas - (2 if direct else 3))
            own_head.start()
            load_text.wait()
            values = text[...].astype(f32)
            text_inv = lax.rsqrt(jnp.sum(values * values, axis=-1, keepdims=True) + epsilon)
            texts[replica, :, 0:span] = values * text_inv
            texts[replica, :, span:] = jnp.full((1, 128), label_ref[0]).astype(f32)
            exchange(texts, 0, "dp", replica, 0, replicas)

        backward(True, before_send)

    def enter_early():
        @pl.when((section > (-1 if direct else 1)) & (section < last))
        def _():
            pl.semaphore_wait(barrier, sections - 1)
            head_copy().start()

    def enter_late():
        if direct:
            return

        @pl.when(section == 0)
        def _():
            pl.semaphore_wait(barrier, sections - 2)

        @pl.when(section == 1)
        def _():
            pl.semaphore_wait(barrier, sections - 1)
            pl.semaphore_signal(ready, inc=1, device_id={"section": 0}, device_id_type=MESH)

    def late_head():
        if direct:
            return

        @pl.when(section == 0)
        def _():
            pl.semaphore_wait(ready, 1)

        @pl.when(section < 2)
        def _():
            head_copy().start()

    enter_early()
    forward(enter_late, late_head)

    @pl.when((section > 0) & (section < last))
    def _():
        backward(False, lambda: None)

    @pl.when(section == 0)
    def _():
        next_ref[...] = jnp.zeros_like(next_ref)

    @pl.when(section < last)
    def _():
        loss_ref[...] = jnp.zeros_like(loss_ref)

    def forward_relays():
        def go(index, start, size):
            part = cut(start, size)
            forward_detour(index, part).wait_recv()
            forward_pass(part).start()

        each_chunk(go)

    def backward_relays():
        def go(index, carry):
            part = cut(index * unit, unit)
            backward_detour(index, part).wait_recv()
            backward_pass(part).start()
            return carry

        lax.fori_loop(0, shards, go, 0)

    if relays:

        @pl.when(section == backward_relay)
        def _():
            backward_relays()

        if forward_relay != last:

            @pl.when(section == forward_relay)
            def _():
                forward_relays()

    @pl.when(section == last)
    def _():
        load_gain.wait()
        final_gain = gain[...].reshape(1, width)
        mean_row = pooled[...]
        centre, pooled_inv = row_stats(mean_row)
        pooled_std = (mean_row - centre) * pooled_inv
        feats[slot] = (pooled_std * final_gain).astype(bf16).astype(f32)
        if group > 1:
            exchange(feats, 1, "dp", slot, first, group)
        own_head.wait()
        head_arrival.wait_recv()
        if group > 1:
            settle(feats, 1, group).wait_recv()
        columns[slot] = jnp.dot(
            feats[:, 0, :].astype(bf16), heads[...], preferred_element_type=f32
        )
        if group > 1:
            exchange(columns, 2, "dp", slot, first, group)
        settle(texts, 0, replicas).wait_recv()
        all_text = texts[:, 0, 0:span]
        label_column = texts[:, 0, span : span + 1]
        column = lax.broadcasted_iota(jnp.int32, (replicas, replicas), 1)
        targets = jnp.where(label_column == column.astype(f32), 1.0, 0.0)
        if group > 1:
            settle(columns, 2, group).wait_recv()
        if relays and forward_relay == last:
            forward_relays()
        embedding = jnp.concatenate([columns[index] for index in range(group)], axis=1)
        image_inv = lax.rsqrt(jnp.sum(embedding * embedding, axis=-1, keepdims=True) + epsilon)
        image_unit = embedding * image_inv
        member = lax.broadcasted_iota(jnp.int32, (group, 1), 0)
        if replicas == group:
            all_image = image_unit
        else:
            images[replica] = jnp.sum(
                jnp.where(member == slot, image_unit, 0.0), axis=0, keepdims=True
            )
            exchange(images, 3, "dp", replica, 0, replicas)
            settle(images, 3, replicas).wait_recv()
            all_image = images[:, 0, :]
        logits = logit_scale * lax.dot_general(
            all_image,
            all_text,
            (((1,), (1,)), ((), ())),
            precision=lax.Precision.HIGHEST,
            preferred_element_type=f32,
        )
        row_max = jnp.max(logits, axis=1, keepdims=True)
        row_lse = row_max + jnp.log(jnp.sum(jnp.exp(logits - row_max), axis=1, keepdims=True))
        col_max = jnp.max(logits, axis=0, keepdims=True)
        col_lse = col_max + jnp.log(jnp.sum(jnp.exp(logits - col_max), axis=0, keepdims=True))
        d_logits = 0.5 * (
            (jnp.exp(logits - row_lse) - targets) + (jnp.exp(logits - col_lse) - targets)
        )
        if replicas != group:
            pick_row = lax.broadcasted_iota(jnp.int32, (group, replicas), 0) + first
            pick_column = lax.broadcasted_iota(jnp.int32, (group, replicas), 1)
            d_logits = jnp.dot(
                jnp.where(pick_row == pick_column, 1.0, 0.0),
                d_logits,
                precision=lax.Precision.HIGHEST,
                preferred_element_type=f32,
            )
        d_image = logit_scale * jnp.dot(
            d_logits, all_text, precision=lax.Precision.HIGHEST, preferred_element_type=f32
        )
        along = jnp.sum(d_image * image_unit, axis=-1, keepdims=True)
        d_rows[...] = (d_image - image_unit * along) * image_inv
        partial = lax.dot_general(
            d_rows[:, my_columns].astype(bf16),
            heads[...],
            (((1,), (1,)), ((), ())),
            preferred_element_type=f32,
        )
        for index in range(group):
            part_out[index] = partial[index : index + 1, :]

        def send_part(step, carry):
            peer = lax.rem(slot + step, group)
            pltpu.make_async_remote_copy(
                part_out.at[peer],
                part_in.at[slot],
                small_send.at[4],
                small_recv.at[4],
                {"dp": first + peer},
                MESH,
            ).start()
            return carry

        lax.fori_loop(1, group, send_part, 0)
        part_in[slot] = jnp.sum(jnp.where(member == slot, partial, 0.0), axis=0, keepdims=True)
        picked = jnp.sum(logits * targets, axis=1, keepdims=True)
        col_picked = jnp.sum(col_lse * targets, axis=1, keepdims=True)
        loss = 0.5 * (row_lse - picked) + 0.5 * (col_picked - picked)
        loss_ref[...] = jnp.broadcast_to(
            jnp.sum(loss, axis=0, keepdims=True) / replicas, loss_ref.shape
        )
        if group > 1:
            settle(part_in, 4, group).wait_recv()
        d_std = jnp.sum(part_in[...], axis=0) * final_gain
        d_pooled = pooled_inv * (
            d_std
            - jnp.sum(d_std, axis=-1, keepdims=True) / width
            - pooled_std * (jnp.sum(d_std * pooled_std, axis=-1, keepdims=True) / width)
        )
        grad_ref[...] = jnp.broadcast_to(d_pooled / tokens, (tokens, width)).astype(bf16)
        settle(texts, 0, replicas).wait_send()
        if group > 1:
            settle(feats, 1, group).wait_send()
            settle(columns, 2, group).wait_send()
            settle(part_out, 4, group).wait_send()
        if replicas != group:
            settle(images, 3, replicas).wait_send()

    @pl.when(section < last)
    def _():
        head_copy().wait_send()
        forward_copy(everything).wait_send()
        backward_copy(everything).wait_recv()

    @pl.when(section > 0)
    def _():
        backward_copy(everything).wait_send()
        forward_copy(everything).wait_recv()

    if relays:

        @pl.when(section == forward_relay)
        def _():
            forward_pass(slice(None)).wait_send()

        @pl.when(section == backward_relay)
        def _():
            backward_pass(slice(None)).wait_send()


def deliver(next_ref, grad_ref, loss_ref, next_out, grad_out, loss_out, sem):
    copies = [
        pltpu.make_async_copy(source, target, sem.at[index])
        for index, (source, target) in enumerate(
            ((next_ref, next_out), (grad_ref, grad_out), (loss_ref, loss_out))
        )
    ]
    for copy in copies:
        copy.start()
    for copy in copies:
        copy.wait()


def in_hbm(value):
    return pltpu.with_memory_space_constraint(value, pltpu.HBM)


def local(
    activations,
    saved,
    cotangents,
    projection,
    section_gain,
    final_gain,
    head_weight,
    text_embed,
    labels,
):
    sections, replicas = lax.axis_size("section"), lax.axis_size("dp")
    tokens, width = activations.shape[2:]
    rows, span = head_weight.shape
    group = math.gcd(replicas, span // 128)
    shard = span // group
    unit = 256 if width % 256 == 0 else 128
    shards = width // unit
    chunks = 1 + (shards - 1) // 2 + (shards - 1) % 2
    f32, bf16 = jnp.float32, jnp.bfloat16
    dma = pltpu.SemaphoreType.DMA
    vmem = pl.BlockSpec(memory_space=pltpu.VMEM)
    hbm = pl.BlockSpec(memory_space=pltpu.HBM)
    big = pltpu.VMEM((tokens, width), bf16)
    next_raw, grad_raw, loss = pl.pallas_call(
        functools.partial(step_kernel, sections, replicas, group, unit),
        out_shape=(big, big, pltpu.VMEM((1, 128), f32)),
        in_specs=[hbm] * 8 + [pl.BlockSpec(memory_space=pltpu.SMEM)],
        out_specs=(vmem, vmem, vmem),
        scratch_shapes=[
            big,
            big,
            big,
            pltpu.VMEM((width, width), bf16),
            big,
            big,
            big,
            pltpu.VMEM((tokens, width), f32),
            pltpu.VMEM((tokens, 128), f32),
            pltpu.VMEM((tokens, 128), f32),
            pltpu.VMEM((1, width), f32),
            pltpu.VMEM((1, width), f32),
            pltpu.VMEM((width,), f32),
            pltpu.VMEM((1, span), bf16),
            pltpu.VMEM((sections * rows, shard), bf16),
            pltpu.VMEM((group, 1, width), f32),
            pltpu.VMEM((group, group, shard), f32),
            pltpu.VMEM((replicas, 1, span), f32),
            pltpu.VMEM((replicas, 1, span + 128), f32),
            pltpu.VMEM((group, span), f32),
            pltpu.VMEM((group, 1, width), f32),
            pltpu.VMEM((group, 1, width), f32),
            big,
            dma((7,)),
            dma((chunks,)),
            dma((2,)),
            dma((3,)),
            dma((2,)),
            dma((shards,)),
            dma((5,)),
            dma((5,)),
            pltpu.SemaphoreType.REGULAR,
        ],
        compiler_params=pltpu.CompilerParams(
            collective_id=0, has_side_effects=True, vmem_limit_bytes=40 * 1024 * 1024
        ),
        name="tower_step",
    )(
        in_hbm(activations[0, 0]),
        in_hbm(saved[0, 0]),
        in_hbm(cotangents[0, 0]),
        in_hbm(projection[0]),
        in_hbm(head_weight),
        in_hbm(section_gain),
        in_hbm(final_gain),
        in_hbm(text_embed),
        labels,
    )
    out = pltpu.HBM((tokens, width), bf16)
    next_act, next_grad, mean_loss = pl.pallas_call(
        deliver,
        out_shape=(out, out, pltpu.HBM((1, 128), f32)),
        in_specs=[vmem, vmem, vmem],
        out_specs=(hbm, hbm, hbm),
        scratch_shapes=[dma((3,))],
        name="deliver",
    )(
        pltpu.with_memory_space_constraint(next_raw, pltpu.VMEM),
        pltpu.with_memory_space_constraint(grad_raw, pltpu.VMEM),
        pltpu.with_memory_space_constraint(loss, pltpu.VMEM),
    )
    return (next_act[None, None], next_grad[None, None], mean_loss[0, :1])


def solution(mesh):
    return jax.shard_map(
        local,
        mesh=mesh,
        in_specs=(
            P("section", "dp", None, None),
            P("section", "dp", None, None),
            P("section", "dp", None, None),
            P("section", None, None),
            P("section", None),
            P(),
            P("section", None),
            P("dp", None),
            P("dp"),
        ),
        out_specs=(P("section", "dp", None, None), P("section", "dp", None, None), P("section")),
        check_vma=False,
    )
```

```python
import functools
import math

import jax
import jax.numpy as jnp
from jax import lax
from jax.experimental import pallas as pl
from jax.experimental.pallas import tpu as pltpu
from jax.sharding import PartitionSpec as P

epsilon = 1e-06
logit_scale = 100.0
MESH = pl.DeviceIdType.MESH
narrow_share = 0.60
wide_share = 0.60
backward_share = 0.5


def row_stats(values):
    width = values.shape[-1]
    centre = jnp.sum(values, axis=-1, keepdims=True) / width
    centred = values - centre
    variance = jnp.sum(centred * centred, axis=-1, keepdims=True) / width
    return centre, lax.rsqrt(variance + epsilon)


def step_kernel(
    sections,
    replicas,
    group,
    unit,
    act_ref,
    saved_ref,
    cot_ref,
    weight_ref,
    head_ref,
    scale_ref,
    gain_ref,
    text_ref,
    label_ref,
    next_ref,
    grad_ref,
    loss_ref,
    act,
    saved,
    cot,
    weight,
    normed,
    block,
    d_input,
    slope,
    sum_slope,
    sum_product,
    pooled,
    scale,
    gain,
    text,
    heads,
    feats,
    columns,
    images,
    texts,
    d_rows,
    part_out,
    part_in,
    relay,
    load_sem,
    weight_sem,
    head_sem,
    bulk_send,
    bulk_recv,
    relay_recv,
    small_send,
    small_recv,
    ready,
):
    section, replica = lax.axis_index("section"), lax.axis_index("dp")
    last = sections - 1
    tokens, width = act.shape
    rows, span = head_ref.shape
    shards = width // unit
    pairs = (shards - 1) // 2
    slot = lax.rem(replica, group)
    first = replica - slot
    shard = span // group
    f32, bf16 = jnp.float32, jnp.bfloat16
    wide = 2 * unit
    lead = [(0, unit)]
    tail = [(unit + pairs * wide, width - unit - pairs * wide)] if (shards - 1) % 2 else []
    n_chunks = 1 + pairs + len(tail)

    def cut(start, size):
        return pl.ds(start if isinstance(start, int) else pl.multiple_of(start, unit), size)

    def each_chunk(step):
        step(0, 0, unit)
        if pairs:

            def go(index, carry):
                step(index + 1, unit + index * wide, wide)
                return carry

            lax.fori_loop(0, pairs, go, 0)
        for start, size in tail:
            step(n_chunks - 1, start, size)

    static_chunks = (
        lead + [(unit + index * wide, wide) for index in range(pairs)] + tail
    )

    def column_load(index, start, size):
        part = cut(start, size)
        return pltpu.make_async_copy(
            weight_ref.at[:, part], weight.at[:, part], weight_sem.at[index]
        )

    def row_load(index, start, size):
        part = cut(start, size)
        return pltpu.make_async_copy(
            weight_ref.at[part, :], weight.at[part, :], weight_sem.at[index]
        )

    def rows_at(share):
        edge = int(tokens * share) // 8 * 8
        return pl.ds(0, edge), pl.ds(edge, tokens - edge)

    narrow_rows, wide_rows = rows_at(narrow_share), rows_at(wide_share)

    def load_act(part):
        picked = narrow_rows[part]
        return pltpu.make_async_copy(
            act_ref.at[picked, :], act.at[picked, :], load_sem.at[(0, 6)[part]]
        )

    load_saved = pltpu.make_async_copy(saved_ref, saved, load_sem.at[1])
    load_cot = pltpu.make_async_copy(cot_ref, cot, load_sem.at[2])
    load_scale = pltpu.make_async_copy(scale_ref, scale, load_sem.at[3])
    load_gain = pltpu.make_async_copy(gain_ref, gain, load_sem.at[4])
    load_text = pltpu.make_async_copy(text_ref, text, load_sem.at[5])

    my_columns = pl.ds(pl.multiple_of(slot * shard, shard), shard)
    own_rows = pl.ds(pl.multiple_of(section * rows, rows), rows)
    own_head = pltpu.make_async_copy(
        head_ref.at[:, my_columns], heads.at[own_rows, :], head_sem.at[2]
    )

    barrier = pltpu.get_barrier_semaphore()

    def greet(axis, me, peers, skip):
        def go(step, carry):
            peer = lax.rem(me + step, peers)

            @pl.when(jnp.abs(me - peer) != skip)
            def _():
                pl.semaphore_signal(barrier, inc=1, device_id={axis: peer}, device_id_type=MESH)

            return carry

        lax.fori_loop(1, peers, go, 0)

    @pl.when(section < last)
    def _():
        load_act(0).start()
        load_scale.start()
        column_load(0, *static_chunks[0]).start()
        own_head.start()
        load_act(1).start()

    def other_loads():
        for index, (start, size) in list(enumerate(static_chunks))[1:]:
            column_load(index, start, size).start()

        @pl.when(section > 0)
        def _():
            load_saved.start()
            load_cot.start()

    @pl.when(section == last)
    def _():
        load_saved.start()
        load_cot.start()
        load_scale.start()
        for index, (start, size) in enumerate(static_chunks):
            row_load(index, start, size).start()
        load_act(0).start()
        load_act(1).start()
        load_text.start()
        load_gain.start()
        own_head.start()

    direct = sections < 4
    greet("section", section, sections, sections if direct else last)

    @pl.when(section == last)
    def _():
        greet("dp", replica, replicas, replicas)

    away = pl.ds(0, last * rows)

    def head_copy():
        return pltpu.make_async_remote_copy(
            heads.at[own_rows, :],
            heads.at[own_rows, :],
            head_sem.at[0],
            head_sem.at[1],
            {"section": last},
            MESH,
        )

    head_arrival = pltpu.make_async_remote_copy(
        heads.at[away, :], heads.at[away, :], head_sem.at[0], head_sem.at[1], {"section": 0}, MESH
    )

    def send_head():
        own_head.wait()
        head_copy().start()

    everything = (slice(None), slice(None))
    forward_send, backward_send, pass_send = bulk_send.at[0], bulk_send.at[1], bulk_send.at[2]
    forward_recv, backward_recv = bulk_recv.at[0], bulk_recv.at[1]

    def move(source, target, send, recv, peer, part):
        return pltpu.make_async_remote_copy(
            source.at[part], target.at[part], send, recv, {"section": peer}, MESH
        )

    def forward_copy(part):
        return move(block, next_ref, forward_send, forward_recv, section + 1, part)

    def backward_copy(part):
        return move(d_input, grad_ref, backward_send, backward_recv, section - 1, part)

    middle = sections // 2
    relays = sections >= 4
    forward_relay, backward_relay = middle + 1, middle - 2

    backward_near, backward_far = rows_at(backward_share)

    def forward_rows(index):
        return narrow_rows if isinstance(index, int) and index == 0 else wide_rows

    def forward_detour(index, columns_part):
        return move(
            block,
            relay,
            forward_send,
            relay_recv.at[index],
            forward_relay,
            (forward_rows(index)[1], columns_part),
        )

    def backward_detour(index, columns_part):
        return move(
            d_input,
            relay,
            backward_send,
            relay_recv.at[index],
            backward_relay,
            (backward_far, columns_part),
        )

    def forward_pass(index, columns_part):
        return move(
            relay,
            next_ref,
            pass_send,
            forward_recv,
            middle,
            (forward_rows(index)[1], columns_part),
        )

    def backward_pass(columns_part):
        return move(
            relay, grad_ref, pass_send, backward_recv, middle - 1, (backward_far, columns_part)
        )

    def send_backward(index, columns_part):
        if not relays:
            backward_copy((slice(None), columns_part)).start()
            return

        @pl.when(section == middle)
        def _():
            backward_copy((backward_near, columns_part)).start()
            backward_detour(index, columns_part).start()

        @pl.when(section != middle)
        def _():
            backward_copy((slice(None), columns_part)).start()

    held = relays and n_chunks > 1 and middle > 1

    def send_held():
        part = cut(*static_chunks[-1])
        forward_copy((forward_rows(1)[0], part)).start()

    def send_forward(index, columns_part, part):
        picked = forward_rows(index)[part]
        if part == 0 and held and not (isinstance(index, int) and index == 0):

            @pl.when((section != middle - 1) | (index != n_chunks - 1))
            def _():
                forward_copy((picked, columns_part)).start()

            return
        if part == 0 or not relays:
            forward_copy((picked, columns_part)).start()
            return

        @pl.when(section == middle - 1)
        def _():
            forward_detour(index, columns_part).start()

        @pl.when(section != middle - 1)
        def _():
            forward_copy((picked, columns_part)).start()

    def normalise(part):
        picked = narrow_rows[part]
        load_act(part).wait()
        if part == 0:

            @pl.when(section < last)
            def _():
                other_loads()

        values = act[picked, :].astype(f32)
        centre, inverse = row_stats(values)
        if part == 0:

            @pl.when(section < last)
            def _():
                load_scale.wait()

        normed[picked, :] = ((values - centre) * inverse * scale[...]).astype(bf16)

    def mix(picked, columns_part):
        mixed = jnp.dot(
            normed[picked, :], weight[:, columns_part], preferred_element_type=f32
        )
        piece = (act[picked, columns_part].astype(f32) + mixed).astype(bf16)
        block[picked, columns_part] = piece
        return jnp.sum(piece.astype(f32), axis=0, keepdims=True)

    def forward(before, between):
        narrow = cut(*lead[0])
        total = jnp.zeros((1, unit), f32)
        for part in range(2):
            normalise(part)
            if part == 0:

                @pl.when(section < last)
                def _():
                    column_load(0, *lead[0]).wait()

            total = total + mix(narrow_rows[part], narrow)
            if part == 0:
                before()

            @pl.when(section < last)
            def _():
                send_forward(0, narrow, part)

        pooled[:, narrow] = total / tokens
        between()

        def step(index, start, size):
            columns_part = cut(start, size)

            @pl.when(section < last)
            def _():
                column_load(index, start, size).wait()

            pooled[:, columns_part] = mix(slice(None), columns_part) / tokens

            @pl.when(section < last)
            def _():
                if relays:
                    for part in range(2):
                        send_forward(index, columns_part, part)
                else:
                    forward_copy((slice(None), columns_part)).start()

        if pairs:

            def go(index, carry):
                step(index + 1, unit + index * wide, wide)
                return carry

            lax.fori_loop(0, pairs, go, 0)
        for start, size in tail:
            step(n_chunks - 1, start, size)

    def folded(values):
        total = values[:, 0:128]
        for start in range(128, values.shape[-1], 128):
            total = total + values[:, start : start + 128]
        return total

    def relay_forward(index, part):
        forward_detour(index, part).wait_recv()
        forward_pass(index, part).start()

    def backward(wait_rows, before_send):
        load_saved.wait()
        centre, inverse = row_stats(saved[...].astype(f32))
        load_cot.wait()
        if wait_rows:
            load_scale.wait()
        sum_slope[...] = jnp.zeros_like(sum_slope)
        sum_product[...] = jnp.zeros_like(sum_product)

        def step(index, start, size):
            part = cut(start, size)
            if wait_rows:
                row_load(index, start, size).wait()
            d_normed = lax.dot_general(
                cot[...],
                weight[part, :],
                (((1,), (1,)), ((), ())),
                preferred_element_type=f32,
            )
            piece = d_normed * scale[:, part]
            slope[:, part] = piece
            sum_slope[...] += folded(piece)
            sum_product[...] += folded(piece * (saved[:, part].astype(f32) - centre))

        if wait_rows:
            for index, (start, size) in enumerate(static_chunks):
                step(index, start, size)
        else:
            each_chunk(step)
        mean_slope = jnp.sum(sum_slope[...], axis=-1, keepdims=True) / width
        mean_product = inverse * (jnp.sum(sum_product[...], axis=-1, keepdims=True) / width)
        offset = inverse * mean_slope
        factor = inverse * inverse * mean_product
        before_send()

        def emit(index, carry):
            part = cut(index * unit, unit)
            d_input[:, part] = (
                cot[:, part].astype(f32)
                + (
                    (inverse * slope[:, part] - offset)
                    - (saved[:, part].astype(f32) - centre) * factor
                )
            ).astype(bf16)
            send_backward(index, part)
            return carry

        lax.fori_loop(0, shards, emit, 0)

    def exchange(slots, pair, axis, me, base, peers):
        def go(step, carry):
            peer = lax.rem(me + step, peers)
            pltpu.make_async_remote_copy(
                slots.at[me],
                slots.at[me],
                small_send.at[pair],
                small_recv.at[pair],
                {axis: base + peer},
                MESH,
            ).start()
            return carry

        lax.fori_loop(1, peers, go, 0)

    def settle(slots, pair, peers):
        others = slots.at[pl.ds(0, peers - 1)]
        return pltpu.make_async_remote_copy(
            others, others, small_send.at[pair], small_recv.at[pair], {"dp": 0}, MESH
        )

    @pl.when(section == last)
    def _():
        def before_send():
            pl.semaphore_wait(barrier, sections + replicas - (2 if direct else 3))
            load_text.wait()
            values = text[...].astype(f32)
            text_inv = lax.rsqrt(jnp.sum(values * values, axis=-1, keepdims=True) + epsilon)
            texts[replica, :, 0:span] = values * text_inv
            texts[replica, :, span:] = jnp.full((1, 128), label_ref[0]).astype(f32)
            exchange(texts, 0, "dp", replica, 0, replicas)

        backward(True, before_send)

    def enter_early():
        @pl.when((section > (-1 if direct else 1)) & (section < last))
        def _():
            pl.semaphore_wait(barrier, sections - 1)
            send_head()

    def enter_late():
        if direct:
            return

        @pl.when(section == 0)
        def _():
            pl.semaphore_wait(barrier, sections - 2)

        @pl.when(section == 1)
        def _():
            pl.semaphore_wait(barrier, sections - 1)
            pl.semaphore_signal(ready, inc=1, device_id={"section": 0}, device_id_type=MESH)

    def late_head():
        if direct:
            return

        @pl.when(section == 0)
        def _():
            pl.semaphore_wait(ready, 1)

        @pl.when(section < 2)
        def _():
            send_head()

    enter_early()
    forward(enter_late, late_head)

    @pl.when((section > 0) & (section < last))
    def _():
        backward(False, lambda: None)
        if held:

            @pl.when(section == middle - 1)
            def _():
                send_held()

    @pl.when(section == 0)
    def _():
        next_ref[...] = jnp.zeros_like(next_ref)

    @pl.when(section < last)
    def _():
        loss_ref[...] = jnp.zeros_like(loss_ref)

    def forward_relays(skip):
        for index, (start, size) in list(enumerate(static_chunks))[skip:]:
            relay_forward(index, cut(start, size))

    def backward_relays():
        def go(index, carry):
            part = cut(index * unit, unit)
            backward_detour(index, part).wait_recv()
            backward_pass(part).start()
            return carry

        lax.fori_loop(0, shards, go, 0)

    if relays:

        @pl.when(section == backward_relay)
        def _():
            backward_relays()

        if forward_relay != last:

            @pl.when(section == forward_relay)
            def _():
                forward_relays(0)

    @pl.when(section == last)
    def _():
        load_gain.wait()
        final_gain = gain[...].reshape(1, width)
        mean_row = pooled[...]
        centre, pooled_inv = row_stats(mean_row)
        pooled_std = (mean_row - centre) * pooled_inv
        feats[slot] = (pooled_std * final_gain).astype(bf16).astype(f32)
        if group > 1:
            exchange(feats, 1, "dp", slot, first, group)
        own_head.wait()
        head_arrival.wait_recv()
        if group > 1:
            settle(feats, 1, group).wait_recv()
        columns[slot] = jnp.dot(
            feats[:, 0, :].astype(bf16), heads[...], preferred_element_type=f32
        )
        if group > 1:
            exchange(columns, 2, "dp", slot, first, group)
        settle(texts, 0, replicas).wait_recv()
        all_text = texts[:, 0, 0:span]
        label_column = texts[:, 0, span : span + 1]
        column = lax.broadcasted_iota(jnp.int32, (replicas, replicas), 1)
        targets = jnp.where(label_column == column.astype(f32), 1.0, 0.0)
        if group > 1:
            settle(columns, 2, group).wait_recv()
        if relays and forward_relay == last:
            forward_relays(0)
        embedding = jnp.concatenate([columns[index] for index in range(group)], axis=1)
        image_inv = lax.rsqrt(jnp.sum(embedding * embedding, axis=-1, keepdims=True) + epsilon)
        image_unit = embedding * image_inv
        member = lax.broadcasted_iota(jnp.int32, (group, 1), 0)
        if replicas == group:
            all_image = image_unit
        else:
            images[replica] = jnp.sum(
                jnp.where(member == slot, image_unit, 0.0), axis=0, keepdims=True
            )
            exchange(images, 3, "dp", replica, 0, replicas)
            settle(images, 3, replicas).wait_recv()
            all_image = images[:, 0, :]
        logits = logit_scale * lax.dot_general(
            all_image,
            all_text,
            (((1,), (1,)), ((), ())),
            precision=lax.Precision.HIGHEST,
            preferred_element_type=f32,
        )
        row_max = jnp.max(logits, axis=1, keepdims=True)
        row_lse = row_max + jnp.log(jnp.sum(jnp.exp(logits - row_max), axis=1, keepdims=True))
        col_max = jnp.max(logits, axis=0, keepdims=True)
        col_lse = col_max + jnp.log(jnp.sum(jnp.exp(logits - col_max), axis=0, keepdims=True))
        d_logits = 0.5 * (
            (jnp.exp(logits - row_lse) - targets) + (jnp.exp(logits - col_lse) - targets)
        )
        if replicas != group:
            pick_row = lax.broadcasted_iota(jnp.int32, (group, replicas), 0) + first
            pick_column = lax.broadcasted_iota(jnp.int32, (group, replicas), 1)
            d_logits = jnp.dot(
                jnp.where(pick_row == pick_column, 1.0, 0.0),
                d_logits,
                precision=lax.Precision.HIGHEST,
                preferred_element_type=f32,
            )
        d_image = logit_scale * jnp.dot(
            d_logits, all_text, precision=lax.Precision.HIGHEST, preferred_element_type=f32
        )
        along = jnp.sum(d_image * image_unit, axis=-1, keepdims=True)
        d_rows[...] = (d_image - image_unit * along) * image_inv
        partial = lax.dot_general(
            d_rows[:, my_columns].astype(bf16),
            heads[...],
            (((1,), (1,)), ((), ())),
            preferred_element_type=f32,
        )
        for index in range(group):
            part_out[index] = partial[index : index + 1, :]

        def send_part(step, carry):
            peer = lax.rem(slot + step, group)
            pltpu.make_async_remote_copy(
                part_out.at[peer],
                part_in.at[slot],
                small_send.at[4],
                small_recv.at[4],
                {"dp": first + peer},
                MESH,
            ).start()
            return carry

        lax.fori_loop(1, group, send_part, 0)
        part_in[slot] = jnp.sum(jnp.where(member == slot, partial, 0.0), axis=0, keepdims=True)
        picked = jnp.sum(logits * targets, axis=1, keepdims=True)
        col_picked = jnp.sum(col_lse * targets, axis=1, keepdims=True)
        loss = 0.5 * (row_lse - picked) + 0.5 * (col_picked - picked)
        loss_ref[...] = jnp.broadcast_to(
            jnp.sum(loss, axis=0, keepdims=True) / replicas, loss_ref.shape
        )
        if group > 1:
            settle(part_in, 4, group).wait_recv()
        d_std = jnp.sum(part_in[...], axis=0) * final_gain
        d_pooled = pooled_inv * (
            d_std
            - jnp.sum(d_std, axis=-1, keepdims=True) / width
            - pooled_std * (jnp.sum(d_std * pooled_std, axis=-1, keepdims=True) / width)
        )
        grad_ref[...] = jnp.broadcast_to(d_pooled / tokens, (tokens, width)).astype(bf16)
        settle(texts, 0, replicas).wait_send()
        if group > 1:
            settle(feats, 1, group).wait_send()
            settle(columns, 2, group).wait_send()
            settle(part_out, 4, group).wait_send()
        if replicas != group:
            settle(images, 3, replicas).wait_send()

    @pl.when(section < last)
    def _():
        head_copy().wait_send()
        forward_copy(everything).wait_send()
        backward_copy(everything).wait_recv()

    @pl.when(section > 0)
    def _():
        backward_copy(everything).wait_send()
        forward_copy(everything).wait_recv()

    if relays:

        @pl.when(section == forward_relay)
        def _():
            for index, (start, size) in enumerate(static_chunks):
                forward_pass(index, cut(start, size)).wait_send()

        @pl.when(section == backward_relay)
        def _():
            backward_pass(slice(None)).wait_send()


def deliver(next_ref, grad_ref, loss_ref, next_out, grad_out, loss_out, sem):
    copies = [
        pltpu.make_async_copy(source, target, sem.at[index])
        for index, (source, target) in enumerate(
            ((next_ref, next_out), (grad_ref, grad_out), (loss_ref, loss_out))
        )
    ]
    for copy in copies:
        copy.start()
    for copy in copies:
        copy.wait()


def in_hbm(value):
    return pltpu.with_memory_space_constraint(value, pltpu.HBM)


def local(
    activations,
    saved,
    cotangents,
    projection,
    section_gain,
    final_gain,
    head_weight,
    text_embed,
    labels,
):
    sections, replicas = lax.axis_size("section"), lax.axis_size("dp")
    tokens, width = activations.shape[2:]
    rows, span = head_weight.shape
    group = math.gcd(replicas, span // 128)
    shard = span // group
    unit = 256 if width % 256 == 0 else 128
    shards = width // unit
    chunks = 1 + (shards - 1) // 2 + (shards - 1) % 2
    f32, bf16 = jnp.float32, jnp.bfloat16
    dma = pltpu.SemaphoreType.DMA
    vmem = pl.BlockSpec(memory_space=pltpu.VMEM)
    hbm = pl.BlockSpec(memory_space=pltpu.HBM)
    big = pltpu.VMEM((tokens, width), bf16)
    next_raw, grad_raw, loss = pl.pallas_call(
        functools.partial(step_kernel, sections, replicas, group, unit),
        out_shape=(big, big, pltpu.VMEM((1, 128), f32)),
        in_specs=[hbm] * 8 + [pl.BlockSpec(memory_space=pltpu.SMEM)],
        out_specs=(vmem, vmem, vmem),
        scratch_shapes=[
            big,
            big,
            big,
            pltpu.VMEM((width, width), bf16),
            big,
            big,
            big,
            pltpu.VMEM((tokens, width), f32),
            pltpu.VMEM((tokens, 128), f32),
            pltpu.VMEM((tokens, 128), f32),
            pltpu.VMEM((1, width), f32),
            pltpu.VMEM((1, width), f32),
            pltpu.VMEM((width,), f32),
            pltpu.VMEM((1, span), bf16),
            pltpu.VMEM((sections * rows, shard), bf16),
            pltpu.VMEM((group, 1, width), f32),
            pltpu.VMEM((group, group, shard), f32),
            pltpu.VMEM((replicas, 1, span), f32),
            pltpu.VMEM((replicas, 1, span + 128), f32),
            pltpu.VMEM((group, span), f32),
            pltpu.VMEM((group, 1, width), f32),
            pltpu.VMEM((group, 1, width), f32),
            big,
            dma((7,)),
            dma((chunks,)),
            dma((3,)),
            dma((3,)),
            dma((2,)),
            dma((shards,)),
            dma((5,)),
            dma((5,)),
            pltpu.SemaphoreType.REGULAR,
        ],
        compiler_params=pltpu.CompilerParams(
            collective_id=0, has_side_effects=True, vmem_limit_bytes=40 * 1024 * 1024
        ),
        name="tower_step",
    )(
        in_hbm(activations[0, 0]),
        in_hbm(saved[0, 0]),
        in_hbm(cotangents[0, 0]),
        in_hbm(projection[0]),
        in_hbm(head_weight),
        in_hbm(section_gain),
        in_hbm(final_gain),
        in_hbm(text_embed),
        labels,
    )
    out = pltpu.HBM((tokens, width), bf16)
    next_act, next_grad, mean_loss = pl.pallas_call(
        deliver,
        out_shape=(out, out, pltpu.HBM((1, 128), f32)),
        in_specs=[vmem, vmem, vmem],
        out_specs=(hbm, hbm, hbm),
        scratch_shapes=[dma((3,))],
        name="deliver",
    )(
        pltpu.with_memory_space_constraint(next_raw, pltpu.VMEM),
        pltpu.with_memory_space_constraint(grad_raw, pltpu.VMEM),
        pltpu.with_memory_space_constraint(loss, pltpu.VMEM),
    )
    return (next_act[None, None], next_grad[None, None], mean_loss[0, :1])


def solution(mesh):
    return jax.shard_map(
        local,
        mesh=mesh,
        in_specs=(
            P("section", "dp", None, None),
            P("section", "dp", None, None),
            P("section", "dp", None, None),
            P("section", None, None),
            P("section", None),
            P(),
            P("section", None),
            P("dp", None),
            P("dp"),
        ),
        out_specs=(P("section", "dp", None, None), P("section", "dp", None, None), P("section")),
        check_vma=False,
    )
```

```python
import functools
import math

import jax
import jax.numpy as jnp
from jax import lax
from jax.experimental import pallas as pl
from jax.experimental.pallas import tpu as pltpu
from jax.sharding import PartitionSpec as P

epsilon = 1e-06
logit_scale = 100.0
MESH = pl.DeviceIdType.MESH
narrow_share = 0.56
wide_share = 0.60
backward_share = 0.5


def row_stats(values):
    width = values.shape[-1]
    centre = jnp.sum(values, axis=-1, keepdims=True) / width
    centred = values - centre
    variance = jnp.sum(centred * centred, axis=-1, keepdims=True) / width
    return centre, lax.rsqrt(variance + epsilon)


def step_kernel(
    sections,
    replicas,
    group,
    unit,
    act_ref,
    saved_ref,
    cot_ref,
    weight_ref,
    head_ref,
    scale_ref,
    gain_ref,
    text_ref,
    label_ref,
    next_ref,
    grad_ref,
    loss_ref,
    act,
    saved,
    cot,
    weight,
    normed,
    block,
    d_input,
    slope,
    sum_slope,
    sum_product,
    pooled,
    scale,
    gain,
    text,
    heads,
    feats,
    columns,
    images,
    texts,
    d_rows,
    part_out,
    part_in,
    relay,
    load_sem,
    weight_sem,
    head_sem,
    bulk_send,
    bulk_recv,
    relay_recv,
    small_send,
    small_recv,
    ready,
):
    section, replica = lax.axis_index("section"), lax.axis_index("dp")
    last = sections - 1
    tokens, width = act.shape
    rows, span = head_ref.shape
    shards = width // unit
    pairs = (shards - 1) // 2
    slot = lax.rem(replica, group)
    first = replica - slot
    shard = span // group
    middle = sections // 2
    relays = sections >= 4
    f32, bf16 = jnp.float32, jnp.bfloat16
    wide = 2 * unit
    lead = [(0, unit)]
    tail = [(unit + pairs * wide, width - unit - pairs * wide)] if (shards - 1) % 2 else []
    n_chunks = 1 + pairs + len(tail)

    def cut(start, size):
        return pl.ds(start if isinstance(start, int) else pl.multiple_of(start, unit), size)

    def each_chunk(step):
        step(0, 0, unit)
        if pairs:

            def go(index, carry):
                step(index + 1, unit + index * wide, wide)
                return carry

            lax.fori_loop(0, pairs, go, 0)
        for start, size in tail:
            step(n_chunks - 1, start, size)

    static_chunks = (
        lead + [(unit + index * wide, wide) for index in range(pairs)] + tail
    )

    def column_load(index, start, size):
        part = cut(start, size)
        return pltpu.make_async_copy(
            weight_ref.at[:, part], weight.at[:, part], weight_sem.at[index]
        )

    def row_load(index, start, size):
        part = cut(start, size)
        return pltpu.make_async_copy(
            weight_ref.at[part, :], weight.at[part, :], weight_sem.at[index]
        )

    def rows_at(share):
        edge = int(tokens * share) // 8 * 8
        return pl.ds(0, edge), pl.ds(edge, tokens - edge)

    narrow_rows, wide_rows = rows_at(narrow_share), rows_at(wide_share)

    def load_act(part):
        picked = narrow_rows[part]
        return pltpu.make_async_copy(
            act_ref.at[picked, :], act.at[picked, :], load_sem.at[(4, 1)[part]]
        )

    load_saved = pltpu.make_async_copy(saved_ref, saved, load_sem.at[0])
    load_cot = pltpu.make_async_copy(cot_ref, cot, load_sem.at[2])
    load_scale = pltpu.make_async_copy(scale_ref, scale, load_sem.at[3])
    load_gain = pltpu.make_async_copy(gain_ref, gain, load_sem.at[2])
    load_text = pltpu.make_async_copy(text_ref, text, load_sem.at[0])

    my_columns = pl.ds(pl.multiple_of(slot * shard, shard), shard)
    own_rows = pl.ds(pl.multiple_of(section * rows, rows), rows)
    own_head = pltpu.make_async_copy(
        head_ref.at[:, my_columns], heads.at[own_rows, :], head_sem.at[0]
    )

    barrier = pltpu.get_barrier_semaphore()

    def greet(axis, me, peers, skip):
        def go(step, carry):
            peer = lax.rem(me + step, peers)

            @pl.when(jnp.abs(me - peer) != skip)
            def _():
                pl.semaphore_signal(barrier, inc=1, device_id={axis: peer}, device_id_type=MESH)

            return carry

        lax.fori_loop(1, peers, go, 0)

    @pl.when(section < last)
    def _():
        load_act(0).start()
        load_scale.start()
        column_load(0, *static_chunks[0]).start()

    @pl.when(section == last)
    def _():
        load_saved.start()
        load_cot.start()
        load_scale.start()
        row_load(0, *static_chunks[0]).start()

    chain = relays
    greet("section", section, sections, last if chain else sections)

    @pl.when(section == last)
    def _():
        greet("dp", replica, replicas, replicas)

    @pl.when(section < last)
    def _():
        own_head.start()
        load_act(1).start()

    def other_loads():
        for index, (start, size) in list(enumerate(static_chunks))[1:]:
            column_load(index, start, size).start()

        @pl.when(section > 0)
        def _():
            load_saved.start()
            load_cot.start()

    @pl.when(section == last)
    def _():
        for index, (start, size) in list(enumerate(static_chunks))[1:]:
            row_load(index, start, size).start()
        load_act(0).start()
        load_act(1).start()
        own_head.start()

    away = pl.ds(0, last * rows)

    def head_copy():
        return pltpu.make_async_remote_copy(
            heads.at[own_rows, :],
            heads.at[own_rows, :],
            head_sem.at[0],
            head_sem.at[1],
            {"section": last},
            MESH,
        )

    head_arrival = pltpu.make_async_remote_copy(
        heads.at[away, :], heads.at[away, :], head_sem.at[0], head_sem.at[1], {"section": 0}, MESH
    )

    def send_head():
        own_head.wait()
        head_copy().start()

    everything = (slice(None), slice(None))
    forward_send, backward_send, pass_send = bulk_send.at[0], bulk_send.at[1], bulk_send.at[2]
    forward_recv, backward_recv = bulk_recv.at[0], bulk_recv.at[1]

    def move(source, target, send, recv, peer, part):
        return pltpu.make_async_remote_copy(
            source.at[part], target.at[part], send, recv, {"section": peer}, MESH
        )

    def forward_copy(part):
        return move(block, next_ref, forward_send, forward_recv, section + 1, part)

    def backward_copy(part):
        return move(d_input, grad_ref, backward_send, backward_recv, section - 1, part)

    forward_relay, backward_relay = middle + 1, middle - 2

    backward_near, backward_far = rows_at(backward_share)

    def forward_rows(index):
        return narrow_rows if isinstance(index, int) and index == 0 else wide_rows

    def forward_detour(index, columns_part):
        return move(
            block,
            relay,
            forward_send,
            relay_recv.at[index],
            forward_relay,
            (forward_rows(index)[1], columns_part),
        )

    def backward_detour(index, columns_part):
        return move(
            d_input,
            relay,
            backward_send,
            relay_recv.at[index],
            backward_relay,
            (backward_far, columns_part),
        )

    def forward_pass(index, columns_part):
        return move(
            relay,
            next_ref,
            pass_send,
            forward_recv,
            middle,
            (forward_rows(index)[1], columns_part),
        )

    def backward_pass(columns_part):
        return move(
            relay, grad_ref, pass_send, backward_recv, middle - 1, (backward_far, columns_part)
        )

    def send_backward(index, columns_part):
        if not relays:
            backward_copy((slice(None), columns_part)).start()
            return

        @pl.when(section == middle)
        def _():
            backward_copy((backward_near, columns_part)).start()
            backward_detour(index, columns_part).start()

        @pl.when(section != middle)
        def _():
            backward_copy((slice(None), columns_part)).start()

    held = relays and n_chunks > 1 and middle > 1

    def send_held():
        part = cut(*static_chunks[-1])
        forward_copy((forward_rows(1)[0], part)).start()

    def send_forward(index, columns_part, part):
        picked = forward_rows(index)[part]
        if part == 0 and held and not (isinstance(index, int) and index == 0):

            @pl.when((section != middle - 1) | (index != n_chunks - 1))
            def _():
                forward_copy((picked, columns_part)).start()

            return
        if part == 0 or not relays:
            forward_copy((picked, columns_part)).start()
            return

        @pl.when(section == middle - 1)
        def _():
            forward_detour(index, columns_part).start()

        @pl.when(section != middle - 1)
        def _():
            forward_copy((picked, columns_part)).start()

    def normalise(part):
        picked = narrow_rows[part]
        load_act(part).wait()
        if part == 0:

            @pl.when(section < last)
            def _():
                other_loads()

        values = act[picked, :].astype(f32)
        centre, inverse = row_stats(values)
        if part == 0:

            @pl.when(section < last)
            def _():
                load_scale.wait()

        normed[picked, :] = ((values - centre) * inverse * scale[...]).astype(bf16)

    def mix(picked, columns_part):
        mixed = jnp.dot(
            normed[picked, :], weight[:, columns_part], preferred_element_type=f32
        )
        piece = (act[picked, columns_part].astype(f32) + mixed).astype(bf16)
        block[picked, columns_part] = piece
        return jnp.sum(piece.astype(f32), axis=0, keepdims=True)

    def forward(before, between):
        narrow = cut(*lead[0])
        total = jnp.zeros((1, unit), f32)
        for part in range(2):
            normalise(part)
            if part == 0:

                @pl.when(section < last)
                def _():
                    column_load(0, *lead[0]).wait()

            total = total + mix(narrow_rows[part], narrow)
            if part == 0:
                before()

            @pl.when(section < last)
            def _():
                send_forward(0, narrow, part)

        pooled[:, narrow] = total / tokens
        between()

        def step(index, start, size):
            columns_part = cut(start, size)

            @pl.when(section < last)
            def _():
                column_load(index, start, size).wait()

            pooled[:, columns_part] = mix(slice(None), columns_part) / tokens

            @pl.when(section < last)
            def _():
                if relays:
                    for part in range(2):
                        send_forward(index, columns_part, part)
                else:
                    forward_copy((slice(None), columns_part)).start()

        if pairs:

            def go(index, carry):
                step(index + 1, unit + index * wide, wide)
                return carry

            lax.fori_loop(0, pairs, go, 0)
        for start, size in tail:
            step(n_chunks - 1, start, size)

    def folded(values):
        total = values[:, 0:128]
        for start in range(128, values.shape[-1], 128):
            total = total + values[:, start : start + 128]
        return total

    def relay_forward(index, part):
        forward_detour(index, part).wait_recv()
        forward_pass(index, part).start()

    def backward(wait_rows, before_send):
        load_saved.wait()
        centre, inverse = row_stats(saved[...].astype(f32))
        load_cot.wait()
        if wait_rows:
            load_text.start()
            load_gain.start()
            load_scale.wait()
        sum_slope[...] = jnp.zeros_like(sum_slope)
        sum_product[...] = jnp.zeros_like(sum_product)

        def step(index, start, size):
            part = cut(start, size)
            if wait_rows:
                row_load(index, start, size).wait()
            d_normed = lax.dot_general(
                cot[...],
                weight[part, :],
                (((1,), (1,)), ((), ())),
                preferred_element_type=f32,
            )
            piece = d_normed * scale[:, part]
            slope[:, part] = piece
            sum_slope[...] += folded(piece)
            sum_product[...] += folded(piece * (saved[:, part].astype(f32) - centre))

        if wait_rows:
            for index, (start, size) in enumerate(static_chunks):
                step(index, start, size)
        else:
            each_chunk(step)
        mean_slope = jnp.sum(sum_slope[...], axis=-1, keepdims=True) / width
        mean_product = inverse * (jnp.sum(sum_product[...], axis=-1, keepdims=True) / width)
        offset = inverse * mean_slope
        factor = inverse * inverse * mean_product
        before_send()

        def emit(index, start, size):
            part = cut(start, size)
            d_input[:, part] = (
                cot[:, part].astype(f32)
                + (
                    (inverse * slope[:, part] - offset)
                    - (saved[:, part].astype(f32) - centre) * factor
                )
            ).astype(bf16)
            send_backward(index, part)

        each_chunk(emit)

    def exchange(slots, pair, axis, me, base, peers):
        def go(step, carry):
            peer = lax.rem(me + step, peers)
            pltpu.make_async_remote_copy(
                slots.at[me],
                slots.at[me],
                small_send.at[pair],
                small_recv.at[pair],
                {axis: base + peer},
                MESH,
            ).start()
            return carry

        lax.fori_loop(1, peers, go, 0)

    def settle(slots, pair, peers):
        others = slots.at[pl.ds(0, peers - 1)]
        return pltpu.make_async_remote_copy(
            others, others, small_send.at[pair], small_recv.at[pair], {"dp": 0}, MESH
        )

    @pl.when(section == last)
    def _():
        def before_send():
            pl.semaphore_wait(barrier, sections + replicas - (3 if chain else 2))
            load_text.wait()
            values = text[...].astype(f32)
            text_inv = lax.rsqrt(jnp.sum(values * values, axis=-1, keepdims=True) + epsilon)
            texts[replica, :, 0:span] = values * text_inv
            texts[replica, :, span:] = jnp.full((1, 128), label_ref[0]).astype(f32)
            exchange(texts, 0, "dp", replica, 0, replicas)

        backward(True, before_send)

    def tell_first():
        @pl.when(section == 1)
        def _():
            pl.semaphore_signal(ready, inc=1, device_id={"section": 0}, device_id_type=MESH)

    late = (section == 0) | (section == middle - 1) if chain else section < 0

    @pl.when(jnp.logical_not(late) & (section < last))
    def _():
        pl.semaphore_wait(barrier, sections - 1)
        if chain:
            tell_first()
        send_head()

    def enter_late():
        if not chain:
            return

        @pl.when(section == 0)
        def _():
            pl.semaphore_wait(barrier, sections - 2)

        @pl.when(section == middle - 1)
        def _():
            pl.semaphore_wait(barrier, sections - 1)
            tell_first()

    def late_head():
        if not chain:
            return

        @pl.when(section == 0)
        def _():
            pl.semaphore_wait(ready, 1)

        @pl.when(late)
        def _():
            send_head()

    forward(enter_late, late_head)

    @pl.when((section > 0) & (section < last))
    def _():
        backward(False, lambda: None)
        if held:

            @pl.when(section == middle - 1)
            def _():
                send_held()

    @pl.when(section == 0)
    def _():
        next_ref[...] = jnp.zeros_like(next_ref)

    @pl.when(section < last)
    def _():
        loss_ref[...] = jnp.zeros_like(loss_ref)

    def forward_relays(skip):
        for index, (start, size) in list(enumerate(static_chunks))[skip:]:
            relay_forward(index, cut(start, size))

    def backward_relays():
        def go(index, start, size):
            part = cut(start, size)
            backward_detour(index, part).wait_recv()
            backward_pass(part).start()

        each_chunk(go)

    if relays:

        @pl.when(section == backward_relay)
        def _():
            backward_relays()

        if forward_relay != last:

            @pl.when(section == forward_relay)
            def _():
                forward_relays(0)

    @pl.when(section == last)
    def _():
        load_gain.wait()
        final_gain = gain[...].reshape(1, width)
        mean_row = pooled[...]
        centre, pooled_inv = row_stats(mean_row)
        pooled_std = (mean_row - centre) * pooled_inv
        feats[slot] = (pooled_std * final_gain).astype(bf16).astype(f32)
        if group > 1:
            exchange(feats, 1, "dp", slot, first, group)
        own_head.wait()
        head_arrival.wait_recv()
        if group > 1:
            settle(feats, 1, group).wait_recv()
        columns[slot] = jnp.dot(
            feats[:, 0, :].astype(bf16), heads[...], preferred_element_type=f32
        )
        if group > 1:
            exchange(columns, 2, "dp", slot, first, group)
        settle(texts, 0, replicas).wait_recv()
        all_text = texts[:, 0, 0:span]
        label_column = texts[:, 0, span : span + 1]
        column = lax.broadcasted_iota(jnp.int32, (replicas, replicas), 1)
        targets = jnp.where(label_column == column.astype(f32), 1.0, 0.0)
        if group > 1:
            settle(columns, 2, group).wait_recv()
        if relays and forward_relay == last:
            forward_relays(0)
        embedding = jnp.concatenate([columns[index] for index in range(group)], axis=1)
        image_inv = lax.rsqrt(jnp.sum(embedding * embedding, axis=-1, keepdims=True) + epsilon)
        image_unit = embedding * image_inv
        member = lax.broadcasted_iota(jnp.int32, (group, 1), 0)
        if replicas == group:
            all_image = image_unit
        else:
            images[replica] = jnp.sum(
                jnp.where(member == slot, image_unit, 0.0), axis=0, keepdims=True
            )
            exchange(images, 4, "dp", replica, 0, replicas)
            settle(images, 4, replicas).wait_recv()
            all_image = images[:, 0, :]
        logits = logit_scale * lax.dot_general(
            all_image,
            all_text,
            (((1,), (1,)), ((), ())),
            precision=lax.Precision.HIGHEST,
            preferred_element_type=f32,
        )
        row_max = jnp.max(logits, axis=1, keepdims=True)
        row_lse = row_max + jnp.log(jnp.sum(jnp.exp(logits - row_max), axis=1, keepdims=True))
        col_max = jnp.max(logits, axis=0, keepdims=True)
        col_lse = col_max + jnp.log(jnp.sum(jnp.exp(logits - col_max), axis=0, keepdims=True))
        d_logits = 0.5 * (
            (jnp.exp(logits - row_lse) - targets) + (jnp.exp(logits - col_lse) - targets)
        )
        if replicas != group:
            pick_row = lax.broadcasted_iota(jnp.int32, (group, replicas), 0) + first
            pick_column = lax.broadcasted_iota(jnp.int32, (group, replicas), 1)
            d_logits = jnp.dot(
                jnp.where(pick_row == pick_column, 1.0, 0.0),
                d_logits,
                precision=lax.Precision.HIGHEST,
                preferred_element_type=f32,
            )
        d_image = logit_scale * jnp.dot(
            d_logits, all_text, precision=lax.Precision.HIGHEST, preferred_element_type=f32
        )
        along = jnp.sum(d_image * image_unit, axis=-1, keepdims=True)
        d_rows[...] = (d_image - image_unit * along) * image_inv
        partial = lax.dot_general(
            d_rows[:, my_columns].astype(bf16),
            heads[...],
            (((1,), (1,)), ((), ())),
            preferred_element_type=f32,
        )
        for index in range(group):
            part_out[index] = partial[index : index + 1, :]

        def send_part(step, carry):
            peer = lax.rem(slot + step, group)
            pltpu.make_async_remote_copy(
                part_out.at[peer],
                part_in.at[slot],
                small_send.at[3],
                small_recv.at[3],
                {"dp": first + peer},
                MESH,
            ).start()
            return carry

        lax.fori_loop(1, group, send_part, 0)
        part_in[slot] = jnp.sum(jnp.where(member == slot, partial, 0.0), axis=0, keepdims=True)
        picked = jnp.sum(logits * targets, axis=1, keepdims=True)
        col_picked = jnp.sum(col_lse * targets, axis=1, keepdims=True)
        loss = 0.5 * (row_lse - picked) + 0.5 * (col_picked - picked)
        loss_ref[...] = jnp.broadcast_to(
            jnp.sum(loss, axis=0, keepdims=True) / replicas, loss_ref.shape
        )
        if group > 1:
            settle(part_in, 3, group).wait_recv()
        d_std = jnp.sum(part_in[...], axis=0) * final_gain
        d_pooled = pooled_inv * (
            d_std
            - jnp.sum(d_std, axis=-1, keepdims=True) / width
            - pooled_std * (jnp.sum(d_std * pooled_std, axis=-1, keepdims=True) / width)
        )
        grad_ref[...] = jnp.broadcast_to(d_pooled / tokens, (tokens, width)).astype(bf16)
        settle(texts, 0, replicas).wait_send()
        if group > 1:
            settle(feats, 1, group).wait_send()
            settle(columns, 2, group).wait_send()
            settle(part_out, 3, group).wait_send()
        if replicas != group:
            settle(images, 4, replicas).wait_send()

    @pl.when(section < last)
    def _():
        head_copy().wait_send()
        forward_copy(everything).wait_send()
        backward_copy(everything).wait_recv()

    @pl.when(section > 0)
    def _():
        backward_copy(everything).wait_send()
        forward_copy(everything).wait_recv()

    if relays:

        @pl.when(section == forward_relay)
        def _():
            for index, (start, size) in enumerate(static_chunks):
                forward_pass(index, cut(start, size)).wait_send()

        @pl.when(section == backward_relay)
        def _():
            backward_pass(slice(None)).wait_send()


def deliver(next_ref, grad_ref, loss_ref, next_out, grad_out, loss_out, sem):
    copies = [
        pltpu.make_async_copy(source, target, sem.at[index])
        for index, (source, target) in enumerate(
            ((next_ref, next_out), (grad_ref, grad_out), (loss_ref, loss_out))
        )
    ]
    for copy in copies:
        copy.start()
    for copy in copies:
        copy.wait()


def in_hbm(value):
    return pltpu.with_memory_space_constraint(value, pltpu.HBM)


def local(
    activations,
    saved,
    cotangents,
    projection,
    section_gain,
    final_gain,
    head_weight,
    text_embed,
    labels,
):
    sections, replicas = lax.axis_size("section"), lax.axis_size("dp")
    tokens, width = activations.shape[2:]
    rows, span = head_weight.shape
    group = math.gcd(replicas, span // 128)
    shard = span // group
    unit = 256 if width % 256 == 0 else 128
    shards = width // unit
    chunks = 1 + (shards - 1) // 2 + (shards - 1) % 2
    smalls = 4 if replicas == group else 5
    f32, bf16 = jnp.float32, jnp.bfloat16
    dma = pltpu.SemaphoreType.DMA
    vmem = pl.BlockSpec(memory_space=pltpu.VMEM)
    hbm = pl.BlockSpec(memory_space=pltpu.HBM)
    big = pltpu.VMEM((tokens, width), bf16)
    next_raw, grad_raw, loss = pl.pallas_call(
        functools.partial(step_kernel, sections, replicas, group, unit),
        out_shape=(big, big, pltpu.VMEM((1, 128), f32)),
        in_specs=[hbm] * 8 + [pl.BlockSpec(memory_space=pltpu.SMEM)],
        out_specs=(vmem, vmem, vmem),
        scratch_shapes=[
            big,
            big,
            big,
            pltpu.VMEM((width, width), bf16),
            big,
            big,
            big,
            pltpu.VMEM((tokens, width), f32),
            pltpu.VMEM((tokens, 128), f32),
            pltpu.VMEM((tokens, 128), f32),
            pltpu.VMEM((1, width), f32),
            pltpu.VMEM((1, width), f32),
            pltpu.VMEM((width,), f32),
            pltpu.VMEM((1, span), bf16),
            pltpu.VMEM((sections * rows, shard), bf16),
            pltpu.VMEM((group, 1, width), f32),
            pltpu.VMEM((group, group, shard), f32),
            pltpu.VMEM((replicas, 1, span), f32),
            pltpu.VMEM((replicas, 1, span + 128), f32),
            pltpu.VMEM((group, span), f32),
            pltpu.VMEM((group, 1, width), f32),
            pltpu.VMEM((group, 1, width), f32),
            big,
            dma((5,)),
            dma((chunks,)),
            dma((2,)),
            dma((3,)),
            dma((2,)),
            dma((chunks,)),
            dma((smalls,)),
            dma((smalls,)),
            pltpu.SemaphoreType.REGULAR,
        ],
        compiler_params=pltpu.CompilerParams(
            collective_id=0, has_side_effects=True, vmem_limit_bytes=40 * 1024 * 1024
        ),
        name="tower_step",
    )(
        in_hbm(activations[0, 0]),
        in_hbm(saved[0, 0]),
        in_hbm(cotangents[0, 0]),
        in_hbm(projection[0]),
        in_hbm(head_weight),
        in_hbm(section_gain),
        in_hbm(final_gain),
        in_hbm(text_embed),
        labels,
    )
    out = pltpu.HBM((tokens, width), bf16)
    next_act, next_grad, mean_loss = pl.pallas_call(
        deliver,
        out_shape=(out, out, pltpu.HBM((1, 128), f32)),
        in_specs=[vmem, vmem, vmem],
        out_specs=(hbm, hbm, hbm),
        scratch_shapes=[dma((3,))],
        name="deliver",
    )(
        pltpu.with_memory_space_constraint(next_raw, pltpu.VMEM),
        pltpu.with_memory_space_constraint(grad_raw, pltpu.VMEM),
        pltpu.with_memory_space_constraint(loss, pltpu.VMEM),
    )
    return (next_act[None, None], next_grad[None, None], mean_loss[0, :1])


def solution(mesh):
    return jax.shard_map(
        local,
        mesh=mesh,
        in_specs=(
            P("section", "dp", None, None),
            P("section", "dp", None, None),
            P("section", "dp", None, None),
            P("section", None, None),
            P("section", None),
            P(),
            P("section", None),
            P("dp", None),
            P("dp"),
        ),
        out_specs=(P("section", "dp", None, None), P("section", "dp", None, None), P("section")),
        check_vma=False,
    )
```

```python
import functools
import math

import jax
import jax.numpy as jnp
from jax import lax
from jax.experimental import pallas as pl
from jax.experimental.pallas import tpu as pltpu
from jax.sharding import PartitionSpec as P

epsilon = 1e-06
logit_scale = 100.0
MESH = pl.DeviceIdType.MESH
narrow_share = 0.56
wide_share = 0.60
backward_share = 0.53


def row_stats(values):
    width = values.shape[-1]
    centre = jnp.sum(values, axis=-1, keepdims=True) / width
    centred = values - centre
    variance = jnp.sum(centred * centred, axis=-1, keepdims=True) / width
    return centre, lax.rsqrt(variance + epsilon)


def step_kernel(
    sections,
    replicas,
    group,
    unit,
    act_ref,
    saved_ref,
    cot_ref,
    weight_ref,
    head_ref,
    scale_ref,
    gain_ref,
    text_ref,
    label_ref,
    next_ref,
    grad_ref,
    loss_ref,
    act,
    saved,
    cot,
    weight,
    normed,
    block,
    d_input,
    slope,
    sum_slope,
    sum_product,
    pooled,
    scale,
    gain,
    text,
    heads,
    feats,
    columns,
    images,
    texts,
    d_rows,
    part_out,
    part_in,
    relay,
    load_sem,
    weight_sem,
    head_sem,
    bulk_send,
    bulk_recv,
    relay_recv,
    small_send,
    small_recv,
    ready,
):
    section, replica = lax.axis_index("section"), lax.axis_index("dp")
    last = sections - 1
    tokens, width = act.shape
    rows, span = head_ref.shape
    shards = width // unit
    pairs = (shards - 1) // 2
    slot = lax.rem(replica, group)
    first = replica - slot
    shard = span // group
    middle = sections // 2
    relays = sections >= 4
    f32, bf16 = jnp.float32, jnp.bfloat16
    wide = 2 * unit
    lead = [(0, unit)]
    tail = [(unit + pairs * wide, width - unit - pairs * wide)] if (shards - 1) % 2 else []
    n_chunks = 1 + pairs + len(tail)

    def cut(start, size):
        return pl.ds(start if isinstance(start, int) else pl.multiple_of(start, unit), size)

    def each_chunk(step):
        step(0, 0, unit)
        if pairs:

            def go(index, carry):
                step(index + 1, unit + index * wide, wide)
                return carry

            lax.fori_loop(0, pairs, go, 0)
        for start, size in tail:
            step(n_chunks - 1, start, size)

    static_chunks = (
        lead + [(unit + index * wide, wide) for index in range(pairs)] + tail
    )

    def column_load(index, start, size):
        part = cut(start, size)
        return pltpu.make_async_copy(
            weight_ref.at[:, part], weight.at[:, part], weight_sem.at[index]
        )

    def row_load(index, start, size):
        part = cut(start, size)
        return pltpu.make_async_copy(
            weight_ref.at[part, :], weight.at[part, :], weight_sem.at[index]
        )

    def rows_at(share):
        edge = int(tokens * share) // 8 * 8
        return pl.ds(0, edge), pl.ds(edge, tokens - edge)

    narrow_rows, wide_rows = rows_at(narrow_share), rows_at(wide_share)

    def load_act(part):
        picked = narrow_rows[part]
        return pltpu.make_async_copy(
            act_ref.at[picked, :], act.at[picked, :], load_sem.at[(4, 1)[part]]
        )

    load_saved = pltpu.make_async_copy(saved_ref, saved, load_sem.at[0])
    load_cot = pltpu.make_async_copy(cot_ref, cot, load_sem.at[2])
    load_scale = pltpu.make_async_copy(scale_ref, scale, load_sem.at[3])
    load_gain = pltpu.make_async_copy(gain_ref, gain, load_sem.at[2])
    load_text = pltpu.make_async_copy(text_ref, text, load_sem.at[0])

    my_columns = pl.ds(pl.multiple_of(slot * shard, shard), shard)
    own_rows = pl.ds(pl.multiple_of(section * rows, rows), rows)
    own_head = pltpu.make_async_copy(
        head_ref.at[:, my_columns], heads.at[own_rows, :], head_sem.at[0]
    )

    barrier = pltpu.get_barrier_semaphore()

    def greet(axis, me, peers, skip):
        def go(step, carry):
            peer = lax.rem(me + step, peers)

            @pl.when(jnp.abs(me - peer) != skip)
            def _():
                pl.semaphore_signal(barrier, inc=1, device_id={axis: peer}, device_id_type=MESH)

            return carry

        lax.fori_loop(1, peers, go, 0)

    @pl.when(section < last)
    def _():
        load_act(0).start()
        load_scale.start()
        column_load(0, *static_chunks[0]).start()

    @pl.when(section == last)
    def _():
        load_saved.start()
        load_cot.start()
        load_scale.start()
        row_load(0, *static_chunks[0]).start()

    chain = relays
    greet("section", section, sections, last if chain else sections)

    @pl.when(section == last)
    def _():
        greet("dp", replica, replicas, replicas)

    @pl.when(section < last)
    def _():
        own_head.start()
        load_act(1).start()

    def other_loads():
        for index, (start, size) in list(enumerate(static_chunks))[1:]:
            column_load(index, start, size).start()

        @pl.when(section > 0)
        def _():
            load_saved.start()
            load_cot.start()

    @pl.when(section == last)
    def _():
        for index, (start, size) in list(enumerate(static_chunks))[1:]:
            row_load(index, start, size).start()
        load_act(0).start()
        load_act(1).start()
        own_head.start()

    away = pl.ds(0, last * rows)

    def head_copy():
        return pltpu.make_async_remote_copy(
            heads.at[own_rows, :],
            heads.at[own_rows, :],
            head_sem.at[0],
            head_sem.at[1],
            {"section": last},
            MESH,
        )

    head_arrival = pltpu.make_async_remote_copy(
        heads.at[away, :], heads.at[away, :], head_sem.at[0], head_sem.at[1], {"section": 0}, MESH
    )

    def send_head():
        own_head.wait()
        head_copy().start()

    everything = (slice(None), slice(None))
    forward_send, backward_send, pass_send = bulk_send.at[0], bulk_send.at[1], bulk_send.at[2]
    forward_recv, backward_recv = bulk_recv.at[0], bulk_recv.at[1]

    def move(source, target, send, recv, peer, part):
        return pltpu.make_async_remote_copy(
            source.at[part], target.at[part], send, recv, {"section": peer}, MESH
        )

    def forward_copy(part):
        return move(block, next_ref, forward_send, forward_recv, section + 1, part)

    def backward_copy(part):
        return move(d_input, grad_ref, backward_send, backward_recv, section - 1, part)

    forward_relay, backward_relay = middle + 1, middle - 2

    backward_near, backward_far = rows_at(backward_share)

    def forward_rows(index):
        return narrow_rows if isinstance(index, int) and index == 0 else wide_rows

    def forward_detour(index, columns_part):
        return move(
            block,
            relay,
            forward_send,
            relay_recv.at[index],
            forward_relay,
            (forward_rows(index)[1], columns_part),
        )

    def backward_detour(index, columns_part):
        return move(
            d_input,
            relay,
            backward_send,
            relay_recv.at[index],
            backward_relay,
            (backward_far, columns_part),
        )

    def forward_pass(index, columns_part):
        return move(
            relay,
            next_ref,
            pass_send,
            forward_recv,
            middle,
            (forward_rows(index)[1], columns_part),
        )

    def backward_pass(columns_part):
        return move(
            relay, grad_ref, pass_send, backward_recv, middle - 1, (backward_far, columns_part)
        )

    def send_backward(index, columns_part):
        if not relays:
            backward_copy((slice(None), columns_part)).start()
            return

        @pl.when(section == middle)
        def _():
            backward_copy((backward_near, columns_part)).start()
            backward_detour(index, columns_part).start()

        @pl.when(section != middle)
        def _():
            backward_copy((slice(None), columns_part)).start()

    held = relays and n_chunks > 1

    def keeps(index):
        return ((section == middle - 1) | (section == middle)) & (index == n_chunks - 1)

    def send_held():
        part = cut(*static_chunks[-1])

        @pl.when(section == middle - 1)
        def _():
            forward_copy((forward_rows(1)[0], part)).start()

        @pl.when(section == middle)
        def _():
            forward_copy((slice(None), part)).start()

    def send_forward(index, columns_part, part):
        picked = forward_rows(index)[part]
        if part == 0 and held and not (isinstance(index, int) and index == 0):

            @pl.when(jnp.logical_not(keeps(index)))
            def _():
                forward_copy((picked, columns_part)).start()

            return
        if part == 0 or not relays:
            forward_copy((picked, columns_part)).start()
            return

        @pl.when(section == middle - 1)
        def _():
            forward_detour(index, columns_part).start()

        stays = section != middle - 1
        if held and not (isinstance(index, int) and index == 0):
            stays = stays & jnp.logical_not(keeps(index))

        @pl.when(stays)
        def _():
            forward_copy((picked, columns_part)).start()

    def normalise(part):
        picked = narrow_rows[part]
        load_act(part).wait()
        if part == 0:

            @pl.when(section < last)
            def _():
                other_loads()

        values = act[picked, :].astype(f32)
        centre, inverse = row_stats(values)
        if part == 0:

            @pl.when(section < last)
            def _():
                load_scale.wait()

        normed[picked, :] = ((values - centre) * inverse * scale[...]).astype(bf16)

    def mix(picked, columns_part):
        mixed = jnp.dot(
            normed[picked, :], weight[:, columns_part], preferred_element_type=f32
        )
        piece = (act[picked, columns_part].astype(f32) + mixed).astype(bf16)
        block[picked, columns_part] = piece
        return jnp.sum(piece.astype(f32), axis=0, keepdims=True)

    def forward(before, between):
        narrow = cut(*lead[0])
        total = jnp.zeros((1, unit), f32)
        for part in range(2):
            normalise(part)
            if part == 0:

                @pl.when(section < last)
                def _():
                    column_load(0, *lead[0]).wait()

            total = total + mix(narrow_rows[part], narrow)
            if part == 0:
                before()

            @pl.when(section < last)
            def _():
                send_forward(0, narrow, part)

        pooled[:, narrow] = total / tokens
        between()

        def step(index, start, size):
            columns_part = cut(start, size)

            @pl.when(section < last)
            def _():
                column_load(index, start, size).wait()

            pooled[:, columns_part] = mix(slice(None), columns_part) / tokens

            @pl.when(section < last)
            def _():
                if relays:
                    for part in range(2):
                        send_forward(index, columns_part, part)
                else:
                    forward_copy((slice(None), columns_part)).start()

        if pairs:

            def go(index, carry):
                step(index + 1, unit + index * wide, wide)
                return carry

            lax.fori_loop(0, pairs, go, 0)
        for start, size in tail:
            step(n_chunks - 1, start, size)

    def folded(values):
        total = values[:, 0:128]
        for start in range(128, values.shape[-1], 128):
            total = total + values[:, start : start + 128]
        return total

    def relay_forward(index, part):
        forward_detour(index, part).wait_recv()
        forward_pass(index, part).start()

    def backward(wait_rows, before_send):
        load_saved.wait()
        centre, inverse = row_stats(saved[...].astype(f32))
        load_cot.wait()
        if wait_rows:
            load_text.start()
            load_gain.start()
            load_scale.wait()
        sum_slope[...] = jnp.zeros_like(sum_slope)
        sum_product[...] = jnp.zeros_like(sum_product)

        def step(index, start, size):
            part = cut(start, size)
            if wait_rows:
                row_load(index, start, size).wait()
            d_normed = lax.dot_general(
                cot[...],
                weight[part, :],
                (((1,), (1,)), ((), ())),
                preferred_element_type=f32,
            )
            piece = d_normed * scale[:, part]
            slope[:, part] = piece
            sum_slope[...] += folded(piece)
            sum_product[...] += folded(piece * (saved[:, part].astype(f32) - centre))

        if wait_rows:
            for index, (start, size) in enumerate(static_chunks):
                step(index, start, size)
        else:
            each_chunk(step)
        mean_slope = jnp.sum(sum_slope[...], axis=-1, keepdims=True) / width
        mean_product = inverse * (jnp.sum(sum_product[...], axis=-1, keepdims=True) / width)
        offset = inverse * mean_slope
        factor = inverse * inverse * mean_product
        before_send()

        def emit(index, start, size):
            part = cut(start, size)
            d_input[:, part] = (
                cot[:, part].astype(f32)
                + (
                    (inverse * slope[:, part] - offset)
                    - (saved[:, part].astype(f32) - centre) * factor
                )
            ).astype(bf16)
            send_backward(index, part)

        each_chunk(emit)

    def exchange(slots, pair, axis, me, base, peers):
        def go(step, carry):
            peer = lax.rem(me + step, peers)
            pltpu.make_async_remote_copy(
                slots.at[me],
                slots.at[me],
                small_send.at[pair],
                small_recv.at[pair],
                {axis: base + peer},
                MESH,
            ).start()
            return carry

        lax.fori_loop(1, peers, go, 0)

    def settle(slots, pair, peers):
        others = slots.at[pl.ds(0, peers - 1)]
        return pltpu.make_async_remote_copy(
            others, others, small_send.at[pair], small_recv.at[pair], {"dp": 0}, MESH
        )

    @pl.when(section == last)
    def _():
        def before_send():
            pl.semaphore_wait(barrier, sections + replicas - (3 if chain else 2))
            load_text.wait()
            values = text[...].astype(f32)
            text_inv = lax.rsqrt(jnp.sum(values * values, axis=-1, keepdims=True) + epsilon)
            texts[replica, :, 0:span] = values * text_inv
            texts[replica, :, span:] = jnp.full((1, 128), label_ref[0]).astype(f32)
            exchange(texts, 0, "dp", replica, 0, replicas)

        backward(True, before_send)

    def tell_first():
        @pl.when(section == 1)
        def _():
            pl.semaphore_signal(ready, inc=1, device_id={"section": 0}, device_id_type=MESH)

    late = (section == 0) | (section == middle - 1) if chain else section < 0

    @pl.when(jnp.logical_not(late) & (section < last))
    def _():
        pl.semaphore_wait(barrier, sections - 1)
        if chain:
            tell_first()
        send_head()

    def enter_late():
        if not chain:
            return

        @pl.when(section == 0)
        def _():
            pl.semaphore_wait(barrier, sections - 2)

        @pl.when(section == middle - 1)
        def _():
            pl.semaphore_wait(barrier, sections - 1)
            tell_first()

    def late_head():
        if not chain:
            return

        @pl.when(section == 0)
        def _():
            pl.semaphore_wait(ready, 1)

        @pl.when(late)
        def _():
            send_head()

    forward(enter_late, late_head)

    @pl.when((section > 0) & (section < last))
    def _():
        backward(False, lambda: None)
        if held:

            send_held()

    @pl.when(section == 0)
    def _():
        next_ref[...] = jnp.zeros_like(next_ref)

    @pl.when(section < last)
    def _():
        loss_ref[...] = jnp.zeros_like(loss_ref)

    def forward_relays(skip):
        for index, (start, size) in list(enumerate(static_chunks))[skip:]:
            relay_forward(index, cut(start, size))

    def backward_relays():
        def go(index, start, size):
            part = cut(start, size)
            backward_detour(index, part).wait_recv()
            backward_pass(part).start()

        each_chunk(go)

    if relays:

        @pl.when(section == backward_relay)
        def _():
            backward_relays()

        if forward_relay != last:

            @pl.when(section == forward_relay)
            def _():
                forward_relays(0)

    @pl.when(section == last)
    def _():
        load_gain.wait()
        final_gain = gain[...].reshape(1, width)
        mean_row = pooled[...]
        centre, pooled_inv = row_stats(mean_row)
        pooled_std = (mean_row - centre) * pooled_inv
        feats[slot] = (pooled_std * final_gain).astype(bf16).astype(f32)
        if group > 1:
            exchange(feats, 1, "dp", slot, first, group)
        own_head.wait()
        head_arrival.wait_recv()
        if group > 1:
            settle(feats, 1, group).wait_recv()
        columns[slot] = jnp.dot(
            feats[:, 0, :].astype(bf16), heads[...], preferred_element_type=f32
        )
        if group > 1:
            exchange(columns, 2, "dp", slot, first, group)
        settle(texts, 0, replicas).wait_recv()
        all_text = texts[:, 0, 0:span]
        label_column = texts[:, 0, span : span + 1]
        column = lax.broadcasted_iota(jnp.int32, (replicas, replicas), 1)
        targets = jnp.where(label_column == column.astype(f32), 1.0, 0.0)
        if group > 1:
            settle(columns, 2, group).wait_recv()
        if relays and forward_relay == last:
            forward_relays(0)
        embedding = jnp.concatenate([columns[index] for index in range(group)], axis=1)
        image_inv = lax.rsqrt(jnp.sum(embedding * embedding, axis=-1, keepdims=True) + epsilon)
        image_unit = embedding * image_inv
        member = lax.broadcasted_iota(jnp.int32, (group, 1), 0)
        if replicas == group:
            all_image = image_unit
        else:
            images[replica] = jnp.sum(
                jnp.where(member == slot, image_unit, 0.0), axis=0, keepdims=True
            )
            exchange(images, 4, "dp", replica, 0, replicas)
            settle(images, 4, replicas).wait_recv()
            all_image = images[:, 0, :]
        logits = logit_scale * lax.dot_general(
            all_image,
            all_text,
            (((1,), (1,)), ((), ())),
            precision=lax.Precision.HIGHEST,
            preferred_element_type=f32,
        )
        row_max = jnp.max(logits, axis=1, keepdims=True)
        row_lse = row_max + jnp.log(jnp.sum(jnp.exp(logits - row_max), axis=1, keepdims=True))
        col_max = jnp.max(logits, axis=0, keepdims=True)
        col_lse = col_max + jnp.log(jnp.sum(jnp.exp(logits - col_max), axis=0, keepdims=True))
        d_logits = 0.5 * (
            (jnp.exp(logits - row_lse) - targets) + (jnp.exp(logits - col_lse) - targets)
        )
        if replicas != group:
            pick_row = lax.broadcasted_iota(jnp.int32, (group, replicas), 0) + first
            pick_column = lax.broadcasted_iota(jnp.int32, (group, replicas), 1)
            d_logits = jnp.dot(
                jnp.where(pick_row == pick_column, 1.0, 0.0),
                d_logits,
                precision=lax.Precision.HIGHEST,
                preferred_element_type=f32,
            )
        d_image = logit_scale * jnp.dot(
            d_logits, all_text, precision=lax.Precision.HIGHEST, preferred_element_type=f32
        )
        along = jnp.sum(d_image * image_unit, axis=-1, keepdims=True)
        d_rows[...] = (d_image - image_unit * along) * image_inv
        partial = lax.dot_general(
            d_rows[:, my_columns].astype(bf16),
            heads[...],
            (((1,), (1,)), ((), ())),
            preferred_element_type=f32,
        )
        for index in range(group):
            part_out[index] = partial[index : index + 1, :]

        def send_part(step, carry):
            peer = lax.rem(slot + step, group)
            pltpu.make_async_remote_copy(
                part_out.at[peer],
                part_in.at[slot],
                small_send.at[3],
                small_recv.at[3],
                {"dp": first + peer},
                MESH,
            ).start()
            return carry

        lax.fori_loop(1, group, send_part, 0)
        part_in[slot] = jnp.sum(jnp.where(member == slot, partial, 0.0), axis=0, keepdims=True)
        picked = jnp.sum(logits * targets, axis=1, keepdims=True)
        col_picked = jnp.sum(col_lse * targets, axis=1, keepdims=True)
        loss = 0.5 * (row_lse - picked) + 0.5 * (col_picked - picked)
        loss_ref[...] = jnp.broadcast_to(
            jnp.sum(loss, axis=0, keepdims=True) / replicas, loss_ref.shape
        )
        if group > 1:
            settle(part_in, 3, group).wait_recv()
        d_std = jnp.sum(part_in[...], axis=0) * final_gain
        d_pooled = pooled_inv * (
            d_std
            - jnp.sum(d_std, axis=-1, keepdims=True) / width
            - pooled_std * (jnp.sum(d_std * pooled_std, axis=-1, keepdims=True) / width)
        )
        grad_ref[...] = jnp.broadcast_to(d_pooled / tokens, (tokens, width)).astype(bf16)
        settle(texts, 0, replicas).wait_send()
        if group > 1:
            settle(feats, 1, group).wait_send()
            settle(columns, 2, group).wait_send()
            settle(part_out, 3, group).wait_send()
        if replicas != group:
            settle(images, 4, replicas).wait_send()

    @pl.when(section < last)
    def _():
        head_copy().wait_send()
        forward_copy(everything).wait_send()
        backward_copy(everything).wait_recv()

    @pl.when(section > 0)
    def _():
        backward_copy(everything).wait_send()
        forward_copy(everything).wait_recv()

    if relays:

        @pl.when(section == forward_relay)
        def _():
            for index, (start, size) in enumerate(static_chunks):
                forward_pass(index, cut(start, size)).wait_send()

        @pl.when(section == backward_relay)
        def _():
            backward_pass(slice(None)).wait_send()


def deliver(next_ref, grad_ref, loss_ref, next_out, grad_out, loss_out, sem):
    copies = [
        pltpu.make_async_copy(source, target, sem.at[index])
        for index, (source, target) in enumerate(
            ((next_ref, next_out), (grad_ref, grad_out), (loss_ref, loss_out))
        )
    ]
    for copy in copies:
        copy.start()
    for copy in copies:
        copy.wait()


def in_hbm(value):
    return pltpu.with_memory_space_constraint(value, pltpu.HBM)


def local(
    activations,
    saved,
    cotangents,
    projection,
    section_gain,
    final_gain,
    head_weight,
    text_embed,
    labels,
):
    sections, replicas = lax.axis_size("section"), lax.axis_size("dp")
    tokens, width = activations.shape[2:]
    rows, span = head_weight.shape
    group = math.gcd(replicas, span // 128)
    shard = span // group
    unit = 256 if width % 256 == 0 else 128
    shards = width // unit
    chunks = 1 + (shards - 1) // 2 + (shards - 1) % 2
    smalls = 4 if replicas == group else 5
    f32, bf16 = jnp.float32, jnp.bfloat16
    dma = pltpu.SemaphoreType.DMA
    vmem = pl.BlockSpec(memory_space=pltpu.VMEM)
    hbm = pl.BlockSpec(memory_space=pltpu.HBM)
    big = pltpu.VMEM((tokens, width), bf16)
    next_raw, grad_raw, loss = pl.pallas_call(
        functools.partial(step_kernel, sections, replicas, group, unit),
        out_shape=(big, big, pltpu.VMEM((1, 128), f32)),
        in_specs=[hbm] * 8 + [pl.BlockSpec(memory_space=pltpu.SMEM)],
        out_specs=(vmem, vmem, vmem),
        scratch_shapes=[
            big,
            big,
            big,
            pltpu.VMEM((width, width), bf16),
            big,
            big,
            big,
            pltpu.VMEM((tokens, width), f32),
            pltpu.VMEM((tokens, 128), f32),
            pltpu.VMEM((tokens, 128), f32),
            pltpu.VMEM((1, width), f32),
            pltpu.VMEM((1, width), f32),
            pltpu.VMEM((width,), f32),
            pltpu.VMEM((1, span), bf16),
            pltpu.VMEM((sections * rows, shard), bf16),
            pltpu.VMEM((group, 1, width), f32),
            pltpu.VMEM((group, group, shard), f32),
            pltpu.VMEM((replicas, 1, span), f32),
            pltpu.VMEM((replicas, 1, span + 128), f32),
            pltpu.VMEM((group, span), f32),
            pltpu.VMEM((group, 1, width), f32),
            pltpu.VMEM((group, 1, width), f32),
            big,
            dma((5,)),
            dma((chunks,)),
            dma((2,)),
            dma((3,)),
            dma((2,)),
            dma((chunks,)),
            dma((smalls,)),
            dma((smalls,)),
            pltpu.SemaphoreType.REGULAR,
        ],
        compiler_params=pltpu.CompilerParams(
            collective_id=0, has_side_effects=True, vmem_limit_bytes=40 * 1024 * 1024
        ),
        name="tower_step",
    )(
        in_hbm(activations[0, 0]),
        in_hbm(saved[0, 0]),
        in_hbm(cotangents[0, 0]),
        in_hbm(projection[0]),
        in_hbm(head_weight),
        in_hbm(section_gain),
        in_hbm(final_gain),
        in_hbm(text_embed),
        labels,
    )
    out = pltpu.HBM((tokens, width), bf16)
    next_act, next_grad, mean_loss = pl.pallas_call(
        deliver,
        out_shape=(out, out, pltpu.HBM((1, 128), f32)),
        in_specs=[vmem, vmem, vmem],
        out_specs=(hbm, hbm, hbm),
        scratch_shapes=[dma((3,))],
        name="deliver",
    )(
        pltpu.with_memory_space_constraint(next_raw, pltpu.VMEM),
        pltpu.with_memory_space_constraint(grad_raw, pltpu.VMEM),
        pltpu.with_memory_space_constraint(loss, pltpu.VMEM),
    )
    return (next_act[None, None], next_grad[None, None], mean_loss[0, :1])


def solution(mesh):
    return jax.shard_map(
        local,
        mesh=mesh,
        in_specs=(
            P("section", "dp", None, None),
            P("section", "dp", None, None),
            P("section", "dp", None, None),
            P("section", None, None),
            P("section", None),
            P(),
            P("section", None),
            P("dp", None),
            P("dp"),
        ),
        out_specs=(P("section", "dp", None, None), P("section", "dp", None, None), P("section")),
        check_vma=False,
    )
```

```python
import functools
import math

import jax
import jax.numpy as jnp
from jax import lax
from jax.experimental import pallas as pl
from jax.experimental.pallas import tpu as pltpu
from jax.sharding import PartitionSpec as P

epsilon = 1e-06
logit_scale = 100.0
MESH = pl.DeviceIdType.MESH
narrow_share = 0.63
wide_share = 0.60
backward_share = 0.53


def row_stats(values):
    width = values.shape[-1]
    centre = jnp.sum(values, axis=-1, keepdims=True) / width
    centred = values - centre
    variance = jnp.sum(centred * centred, axis=-1, keepdims=True) / width
    return centre, lax.rsqrt(variance + epsilon)


def step_kernel(
    sections,
    replicas,
    group,
    unit,
    act_ref,
    saved_ref,
    cot_ref,
    weight_ref,
    head_ref,
    scale_ref,
    gain_ref,
    text_ref,
    label_ref,
    next_ref,
    grad_ref,
    loss_ref,
    act,
    saved,
    cot,
    weight,
    normed,
    block,
    d_input,
    slope,
    sum_slope,
    sum_product,
    pooled,
    scale,
    gain,
    text,
    heads,
    feats,
    columns,
    images,
    texts,
    d_rows,
    part_out,
    part_in,
    relay,
    load_sem,
    weight_sem,
    head_sem,
    bulk_send,
    bulk_recv,
    relay_recv,
    small_send,
    small_recv,
    ready,
):
    section, replica = lax.axis_index("section"), lax.axis_index("dp")
    last = sections - 1
    tokens, width = act.shape
    rows, span = head_ref.shape
    shards = width // unit
    pairs = (shards - 1) // 2
    slot = lax.rem(replica, group)
    first = replica - slot
    shard = span // group
    middle = sections // 2
    relays = sections >= 4
    f32, bf16 = jnp.float32, jnp.bfloat16
    wide = 2 * unit
    lead = [(0, unit)]
    tail = [(unit + pairs * wide, width - unit - pairs * wide)] if (shards - 1) % 2 else []
    n_chunks = 1 + pairs + len(tail)

    def cut(start, size):
        return pl.ds(start if isinstance(start, int) else pl.multiple_of(start, unit), size)

    def each_chunk(step):
        step(0, 0, unit)
        if pairs:

            def go(index, carry):
                step(index + 1, unit + index * wide, wide)
                return carry

            lax.fori_loop(0, pairs, go, 0)
        for start, size in tail:
            step(n_chunks - 1, start, size)

    static_chunks = (
        lead + [(unit + index * wide, wide) for index in range(pairs)] + tail
    )

    def column_load(index, start, size):
        part = cut(start, size)
        return pltpu.make_async_copy(
            weight_ref.at[:, part], weight.at[:, part], weight_sem.at[index]
        )

    def row_load(index, start, size):
        part = cut(start, size)
        return pltpu.make_async_copy(
            weight_ref.at[part, :], weight.at[part, :], weight_sem.at[index]
        )

    def rows_at(share):
        edge = int(tokens * share) // 8 * 8
        return pl.ds(0, edge), pl.ds(edge, tokens - edge)

    narrow_rows, wide_rows = rows_at(narrow_share), rows_at(wide_share)

    def load_act(part):
        picked = narrow_rows[part]
        return pltpu.make_async_copy(
            act_ref.at[picked, :], act.at[picked, :], load_sem.at[(4, 1)[part]]
        )

    load_saved = pltpu.make_async_copy(saved_ref, saved, load_sem.at[0])
    load_cot = pltpu.make_async_copy(cot_ref, cot, load_sem.at[2])
    load_scale = pltpu.make_async_copy(scale_ref, scale, load_sem.at[3])
    load_gain = pltpu.make_async_copy(gain_ref, gain, load_sem.at[2])
    load_text = pltpu.make_async_copy(text_ref, text, load_sem.at[0])

    my_columns = pl.ds(pl.multiple_of(slot * shard, shard), shard)
    own_rows = pl.ds(pl.multiple_of(section * rows, rows), rows)
    own_head = pltpu.make_async_copy(
        head_ref.at[:, my_columns], heads.at[own_rows, :], head_sem.at[0]
    )

    barrier = pltpu.get_barrier_semaphore()

    def greet(axis, me, peers, skip):
        def go(step, carry):
            peer = lax.rem(me + step, peers)

            @pl.when(jnp.abs(me - peer) != skip)
            def _():
                pl.semaphore_signal(barrier, inc=1, device_id={axis: peer}, device_id_type=MESH)

            return carry

        lax.fori_loop(1, peers, go, 0)

    @pl.when(section < last)
    def _():
        load_act(0).start()
        load_scale.start()
        column_load(0, *static_chunks[0]).start()

    @pl.when(section == last)
    def _():
        load_saved.start()
        load_cot.start()
        load_scale.start()
        row_load(0, *static_chunks[0]).start()

    chain = relays
    greet("section", section, sections, last if chain else sections)

    @pl.when(section == last)
    def _():
        greet("dp", replica, replicas, replicas)

    @pl.when(section < last)
    def _():
        own_head.start()
        load_act(1).start()

    def other_loads():
        for index, (start, size) in list(enumerate(static_chunks))[1:]:
            column_load(index, start, size).start()

        @pl.when(section > 0)
        def _():
            load_saved.start()
            load_cot.start()

    @pl.when(section == last)
    def _():
        for index, (start, size) in list(enumerate(static_chunks))[1:]:
            row_load(index, start, size).start()

    away = pl.ds(0, last * rows)

    def head_copy():
        return pltpu.make_async_remote_copy(
            heads.at[own_rows, :],
            heads.at[own_rows, :],
            head_sem.at[0],
            head_sem.at[1],
            {"section": last},
            MESH,
        )

    head_arrival = pltpu.make_async_remote_copy(
        heads.at[away, :], heads.at[away, :], head_sem.at[0], head_sem.at[1], {"section": 0}, MESH
    )

    def send_head():
        own_head.wait()
        head_copy().start()

    everything = (slice(None), slice(None))
    forward_send, backward_send, pass_send = bulk_send.at[0], bulk_send.at[1], bulk_send.at[2]
    forward_recv, backward_recv = bulk_recv.at[0], bulk_recv.at[1]

    def move(source, target, send, recv, peer, part):
        return pltpu.make_async_remote_copy(
            source.at[part], target.at[part], send, recv, {"section": peer}, MESH
        )

    def forward_copy(part):
        return move(block, next_ref, forward_send, forward_recv, section + 1, part)

    def backward_copy(part):
        return move(d_input, grad_ref, backward_send, backward_recv, section - 1, part)

    forward_relay, backward_relay = middle + 1, middle - 2

    backward_near, backward_far = rows_at(backward_share)

    def forward_rows(index):
        return narrow_rows if isinstance(index, int) and index == 0 else wide_rows

    def forward_detour(index, columns_part):
        return move(
            block,
            relay,
            forward_send,
            relay_recv.at[index],
            forward_relay,
            (forward_rows(index)[1], columns_part),
        )

    def backward_detour(index, columns_part):
        return move(
            d_input,
            relay,
            backward_send,
            relay_recv.at[index],
            backward_relay,
            (backward_far, columns_part),
        )

    def forward_pass(index, columns_part):
        return move(
            relay,
            next_ref,
            pass_send,
            forward_recv,
            middle,
            (forward_rows(index)[1], columns_part),
        )

    def backward_pass(columns_part):
        return move(
            relay, grad_ref, pass_send, backward_recv, middle - 1, (backward_far, columns_part)
        )

    def send_backward(index, columns_part):
        if not relays:
            backward_copy((slice(None), columns_part)).start()
            return

        @pl.when(section == middle)
        def _():
            backward_copy((backward_near, columns_part)).start()
            backward_detour(index, columns_part).start()

        @pl.when(section != middle)
        def _():
            backward_copy((slice(None), columns_part)).start()

    held = relays and n_chunks > 1

    def keeps(index):
        return ((section == middle - 1) | (section == middle)) & (index == n_chunks - 1)

    def send_held():
        part = cut(*static_chunks[-1])

        @pl.when(section == middle - 1)
        def _():
            forward_copy((forward_rows(1)[0], part)).start()

        @pl.when(section == middle)
        def _():
            forward_copy((slice(None), part)).start()

    def send_forward(index, columns_part, part):
        picked = forward_rows(index)[part]
        if part == 0 and held and not (isinstance(index, int) and index == 0):

            @pl.when(jnp.logical_not(keeps(index)))
            def _():
                forward_copy((picked, columns_part)).start()

            return
        if part == 0 or not relays:
            forward_copy((picked, columns_part)).start()
            return

        @pl.when(section == middle - 1)
        def _():
            forward_detour(index, columns_part).start()

        stays = section != middle - 1
        if held and not (isinstance(index, int) and index == 0):
            stays = stays & jnp.logical_not(keeps(index))

        @pl.when(stays)
        def _():
            forward_copy((picked, columns_part)).start()

    def normalise(part):
        picked = narrow_rows[part]
        load_act(part).wait()
        if part == 0:

            @pl.when(section < last)
            def _():
                other_loads()

        values = act[picked, :].astype(f32)
        centre, inverse = row_stats(values)
        if part == 0:

            @pl.when(section < last)
            def _():
                load_scale.wait()

        normed[picked, :] = ((values - centre) * inverse * scale[...]).astype(bf16)

    def mix(picked, columns_part):
        mixed = jnp.dot(
            normed[picked, :], weight[:, columns_part], preferred_element_type=f32
        )
        piece = (act[picked, columns_part].astype(f32) + mixed).astype(bf16)
        block[picked, columns_part] = piece
        return jnp.sum(piece.astype(f32), axis=0, keepdims=True)

    def forward(before, between):
        narrow = cut(*lead[0])
        total = jnp.zeros((1, unit), f32)
        for part in range(2):
            normalise(part)
            if part == 0:

                @pl.when(section < last)
                def _():
                    column_load(0, *lead[0]).wait()

            total = total + mix(narrow_rows[part], narrow)
            if part == 0:
                before()

            @pl.when(section < last)
            def _():
                send_forward(0, narrow, part)

        pooled[:, narrow] = total / tokens
        between()

        def step(index, start, size):
            columns_part = cut(start, size)

            @pl.when(section < last)
            def _():
                column_load(index, start, size).wait()

            pooled[:, columns_part] = mix(slice(None), columns_part) / tokens

            @pl.when(section < last)
            def _():
                if relays:
                    for part in range(2):
                        send_forward(index, columns_part, part)
                else:
                    forward_copy((slice(None), columns_part)).start()

        if pairs:

            def go(index, carry):
                step(index + 1, unit + index * wide, wide)
                return carry

            lax.fori_loop(0, pairs, go, 0)
        for start, size in tail:
            step(n_chunks - 1, start, size)

    def folded(values):
        total = values[:, 0:128]
        for start in range(128, values.shape[-1], 128):
            total = total + values[:, start : start + 128]
        return total

    def relay_forward(index, part):
        forward_detour(index, part).wait_recv()
        forward_pass(index, part).start()

    def backward(wait_rows, before_send):
        load_saved.wait()
        centre, inverse = row_stats(saved[...].astype(f32))
        load_cot.wait()
        if wait_rows:
            load_text.start()
            load_gain.start()
            load_scale.wait()
        sum_slope[...] = jnp.zeros_like(sum_slope)
        sum_product[...] = jnp.zeros_like(sum_product)

        def step(index, start, size):
            part = cut(start, size)
            if wait_rows:
                row_load(index, start, size).wait()
            d_normed = lax.dot_general(
                cot[...],
                weight[part, :],
                (((1,), (1,)), ((), ())),
                preferred_element_type=f32,
            )
            piece = d_normed * scale[:, part]
            slope[:, part] = piece
            sum_slope[...] += folded(piece)
            sum_product[...] += folded(piece * (saved[:, part].astype(f32) - centre))

        if wait_rows:
            for index, (start, size) in enumerate(static_chunks):
                step(index, start, size)
                if index == min(1, n_chunks - 1):
                    load_act(0).start()
                    load_act(1).start()
                    own_head.start()
        else:
            each_chunk(step)
        mean_slope = jnp.sum(sum_slope[...], axis=-1, keepdims=True) / width
        mean_product = inverse * (jnp.sum(sum_product[...], axis=-1, keepdims=True) / width)
        offset = inverse * mean_slope
        factor = inverse * inverse * mean_product
        before_send()

        def emit(index, start, size):
            part = cut(start, size)
            d_input[:, part] = (
                cot[:, part].astype(f32)
                + (
                    (inverse * slope[:, part] - offset)
                    - (saved[:, part].astype(f32) - centre) * factor
                )
            ).astype(bf16)
            send_backward(index, part)

        each_chunk(emit)

    def exchange(slots, pair, axis, me, base, peers):
        def go(step, carry):
            peer = lax.rem(me + step, peers)
            pltpu.make_async_remote_copy(
                slots.at[me],
                slots.at[me],
                small_send.at[pair],
                small_recv.at[pair],
                {axis: base + peer},
                MESH,
            ).start()
            return carry

        lax.fori_loop(1, peers, go, 0)

    def settle(slots, pair, peers):
        others = slots.at[pl.ds(0, peers - 1)]
        return pltpu.make_async_remote_copy(
            others, others, small_send.at[pair], small_recv.at[pair], {"dp": 0}, MESH
        )

    @pl.when(section == last)
    def _():
        def before_send():
            pl.semaphore_wait(barrier, sections + replicas - (3 if chain else 2))
            load_text.wait()
            values = text[...].astype(f32)
            text_inv = lax.rsqrt(jnp.sum(values * values, axis=-1, keepdims=True) + epsilon)
            texts[replica, :, 0:span] = values * text_inv
            texts[replica, :, span:] = jnp.full((1, 128), label_ref[0]).astype(f32)
            exchange(texts, 0, "dp", replica, 0, replicas)

        backward(True, before_send)

    def tell_first():
        @pl.when(section == 1)
        def _():
            pl.semaphore_signal(ready, inc=1, device_id={"section": 0}, device_id_type=MESH)

    late = (section == 0) | (section == middle - 1) if chain else section < 0

    @pl.when(jnp.logical_not(late) & (section < last))
    def _():
        pl.semaphore_wait(barrier, sections - 1)
        if chain:
            tell_first()
        send_head()

    def enter_late():
        if not chain:
            return

        @pl.when(section == 0)
        def _():
            pl.semaphore_wait(barrier, sections - 2)

        @pl.when(section == middle - 1)
        def _():
            pl.semaphore_wait(barrier, sections - 1)
            tell_first()

    def late_head():
        if not chain:
            return

        @pl.when(section == 0)
        def _():
            pl.semaphore_wait(ready, 1)

        @pl.when(late)
        def _():
            send_head()

    forward(enter_late, late_head)

    @pl.when((section > 0) & (section < last))
    def _():
        backward(False, lambda: None)
        if held:

            send_held()

    @pl.when(section == 0)
    def _():
        next_ref[...] = jnp.zeros_like(next_ref)

    @pl.when(section < last)
    def _():
        loss_ref[...] = jnp.zeros_like(loss_ref)

    def forward_relays(skip):
        for index, (start, size) in list(enumerate(static_chunks))[skip:]:
            relay_forward(index, cut(start, size))

    def backward_relays():
        def go(index, start, size):
            part = cut(start, size)
            backward_detour(index, part).wait_recv()
            backward_pass(part).start()

        each_chunk(go)

    if relays:

        @pl.when(section == backward_relay)
        def _():
            backward_relays()

        if forward_relay != last:

            @pl.when(section == forward_relay)
            def _():
                forward_relays(0)

    @pl.when(section == last)
    def _():
        load_gain.wait()
        final_gain = gain[...].reshape(1, width)
        mean_row = pooled[...]
        centre, pooled_inv = row_stats(mean_row)
        pooled_std = (mean_row - centre) * pooled_inv
        feats[slot] = (pooled_std * final_gain).astype(bf16).astype(f32)
        if group > 1:
            exchange(feats, 1, "dp", slot, first, group)
        own_head.wait()
        head_arrival.wait_recv()
        if group > 1:
            settle(feats, 1, group).wait_recv()
        columns[slot] = jnp.dot(
            feats[:, 0, :].astype(bf16), heads[...], preferred_element_type=f32
        )
        if group > 1:
            exchange(columns, 2, "dp", slot, first, group)
        settle(texts, 0, replicas).wait_recv()
        all_text = texts[:, 0, 0:span]
        label_column = texts[:, 0, span : span + 1]
        column = lax.broadcasted_iota(jnp.int32, (replicas, replicas), 1)
        targets = jnp.where(label_column == column.astype(f32), 1.0, 0.0)
        if group > 1:
            settle(columns, 2, group).wait_recv()
        if relays and forward_relay == last:
            forward_relays(0)
        embedding = jnp.concatenate([columns[index] for index in range(group)], axis=1)
        image_inv = lax.rsqrt(jnp.sum(embedding * embedding, axis=-1, keepdims=True) + epsilon)
        image_unit = embedding * image_inv
        member = lax.broadcasted_iota(jnp.int32, (group, 1), 0)
        if replicas == group:
            all_image = image_unit
        else:
            images[replica] = jnp.sum(
                jnp.where(member == slot, image_unit, 0.0), axis=0, keepdims=True
            )
            exchange(images, 4, "dp", replica, 0, replicas)
            settle(images, 4, replicas).wait_recv()
            all_image = images[:, 0, :]
        logits = logit_scale * lax.dot_general(
            all_image,
            all_text,
            (((1,), (1,)), ((), ())),
            precision=lax.Precision.HIGHEST,
            preferred_element_type=f32,
        )
        row_max = jnp.max(logits, axis=1, keepdims=True)
        row_lse = row_max + jnp.log(jnp.sum(jnp.exp(logits - row_max), axis=1, keepdims=True))
        col_max = jnp.max(logits, axis=0, keepdims=True)
        col_lse = col_max + jnp.log(jnp.sum(jnp.exp(logits - col_max), axis=0, keepdims=True))
        d_logits = 0.5 * (
            (jnp.exp(logits - row_lse) - targets) + (jnp.exp(logits - col_lse) - targets)
        )
        if replicas != group:
            pick_row = lax.broadcasted_iota(jnp.int32, (group, replicas), 0) + first
            pick_column = lax.broadcasted_iota(jnp.int32, (group, replicas), 1)
            d_logits = jnp.dot(
                jnp.where(pick_row == pick_column, 1.0, 0.0),
                d_logits,
                precision=lax.Precision.HIGHEST,
                preferred_element_type=f32,
            )
        d_image = logit_scale * jnp.dot(
            d_logits, all_text, precision=lax.Precision.HIGHEST, preferred_element_type=f32
        )
        along = jnp.sum(d_image * image_unit, axis=-1, keepdims=True)
        d_rows[...] = (d_image - image_unit * along) * image_inv
        partial = lax.dot_general(
            d_rows[:, my_columns].astype(bf16),
            heads[...],
            (((1,), (1,)), ((), ())),
            preferred_element_type=f32,
        )
        for index in range(group):
            part_out[index] = partial[index : index + 1, :]

        def send_part(step, carry):
            peer = lax.rem(slot + step, group)
            pltpu.make_async_remote_copy(
                part_out.at[peer],
                part_in.at[slot],
                small_send.at[3],
                small_recv.at[3],
                {"dp": first + peer},
                MESH,
            ).start()
            return carry

        lax.fori_loop(1, group, send_part, 0)
        part_in[slot] = jnp.sum(jnp.where(member == slot, partial, 0.0), axis=0, keepdims=True)
        picked = jnp.sum(logits * targets, axis=1, keepdims=True)
        col_picked = jnp.sum(col_lse * targets, axis=1, keepdims=True)
        loss = 0.5 * (row_lse - picked) + 0.5 * (col_picked - picked)
        loss_ref[...] = jnp.broadcast_to(
            jnp.sum(loss, axis=0, keepdims=True) / replicas, loss_ref.shape
        )
        if group > 1:
            settle(part_in, 3, group).wait_recv()
        d_std = jnp.sum(part_in[...], axis=0) * final_gain
        d_pooled = pooled_inv * (
            d_std
            - jnp.sum(d_std, axis=-1, keepdims=True) / width
            - pooled_std * (jnp.sum(d_std * pooled_std, axis=-1, keepdims=True) / width)
        )
        grad_ref[...] = jnp.broadcast_to(d_pooled / tokens, (tokens, width)).astype(bf16)
        settle(texts, 0, replicas).wait_send()
        if group > 1:
            settle(feats, 1, group).wait_send()
            settle(columns, 2, group).wait_send()
            settle(part_out, 3, group).wait_send()
        if replicas != group:
            settle(images, 4, replicas).wait_send()

    @pl.when(section < last)
    def _():
        head_copy().wait_send()
        forward_copy(everything).wait_send()
        backward_copy(everything).wait_recv()

    @pl.when(section > 0)
    def _():
        backward_copy(everything).wait_send()
        forward_copy(everything).wait_recv()

    if relays:

        @pl.when(section == forward_relay)
        def _():
            for index, (start, size) in enumerate(static_chunks):
                forward_pass(index, cut(start, size)).wait_send()

        @pl.when(section == backward_relay)
        def _():
            backward_pass(slice(None)).wait_send()


def deliver(next_ref, grad_ref, loss_ref, next_out, grad_out, loss_out, sem):
    copies = [
        pltpu.make_async_copy(source, target, sem.at[index])
        for index, (source, target) in enumerate(
            ((next_ref, next_out), (grad_ref, grad_out), (loss_ref, loss_out))
        )
    ]
    for copy in copies:
        copy.start()
    for copy in copies:
        copy.wait()


def in_hbm(value):
    return pltpu.with_memory_space_constraint(value, pltpu.HBM)


def local(
    activations,
    saved,
    cotangents,
    projection,
    section_gain,
    final_gain,
    head_weight,
    text_embed,
    labels,
):
    sections, replicas = lax.axis_size("section"), lax.axis_size("dp")
    tokens, width = activations.shape[2:]
    rows, span = head_weight.shape
    group = math.gcd(replicas, span // 128)
    shard = span // group
    unit = 256 if width % 256 == 0 else 128
    shards = width // unit
    chunks = 1 + (shards - 1) // 2 + (shards - 1) % 2
    smalls = 4 if replicas == group else 5
    f32, bf16 = jnp.float32, jnp.bfloat16
    dma = pltpu.SemaphoreType.DMA
    vmem = pl.BlockSpec(memory_space=pltpu.VMEM)
    hbm = pl.BlockSpec(memory_space=pltpu.HBM)
    big = pltpu.VMEM((tokens, width), bf16)
    next_raw, grad_raw, loss = pl.pallas_call(
        functools.partial(step_kernel, sections, replicas, group, unit),
        out_shape=(big, big, pltpu.VMEM((1, 128), f32)),
        in_specs=[hbm] * 8 + [pl.BlockSpec(memory_space=pltpu.SMEM)],
        out_specs=(vmem, vmem, vmem),
        scratch_shapes=[
            big,
            big,
            big,
            pltpu.VMEM((width, width), bf16),
            big,
            big,
            big,
            pltpu.VMEM((tokens, width), f32),
            pltpu.VMEM((tokens, 128), f32),
            pltpu.VMEM((tokens, 128), f32),
            pltpu.VMEM((1, width), f32),
            pltpu.VMEM((1, width), f32),
            pltpu.VMEM((width,), f32),
            pltpu.VMEM((1, span), bf16),
            pltpu.VMEM((sections * rows, shard), bf16),
            pltpu.VMEM((group, 1, width), f32),
            pltpu.VMEM((group, group, shard), f32),
            pltpu.VMEM((replicas, 1, span), f32),
            pltpu.VMEM((replicas, 1, span + 128), f32),
            pltpu.VMEM((group, span), f32),
            pltpu.VMEM((group, 1, width), f32),
            pltpu.VMEM((group, 1, width), f32),
            big,
            dma((5,)),
            dma((chunks,)),
            dma((2,)),
            dma((3,)),
            dma((2,)),
            dma((chunks,)),
            dma((smalls,)),
            dma((smalls,)),
            pltpu.SemaphoreType.REGULAR,
        ],
        compiler_params=pltpu.CompilerParams(
            collective_id=0, has_side_effects=True, vmem_limit_bytes=40 * 1024 * 1024
        ),
        name="tower_step",
    )(
        in_hbm(activations[0, 0]),
        in_hbm(saved[0, 0]),
        in_hbm(cotangents[0, 0]),
        in_hbm(projection[0]),
        in_hbm(head_weight),
        in_hbm(section_gain),
        in_hbm(final_gain),
        in_hbm(text_embed),
        labels,
    )
    out = pltpu.HBM((tokens, width), bf16)
    next_act, next_grad, mean_loss = pl.pallas_call(
        deliver,
        out_shape=(out, out, pltpu.HBM((1, 128), f32)),
        in_specs=[vmem, vmem, vmem],
        out_specs=(hbm, hbm, hbm),
        scratch_shapes=[dma((3,))],
        name="deliver",
    )(
        pltpu.with_memory_space_constraint(next_raw, pltpu.VMEM),
        pltpu.with_memory_space_constraint(grad_raw, pltpu.VMEM),
        pltpu.with_memory_space_constraint(loss, pltpu.VMEM),
    )
    return (next_act[None, None], next_grad[None, None], mean_loss[0, :1])


def solution(mesh):
    return jax.shard_map(
        local,
        mesh=mesh,
        in_specs=(
            P("section", "dp", None, None),
            P("section", "dp", None, None),
            P("section", "dp", None, None),
            P("section", None, None),
            P("section", None),
            P(),
            P("section", None),
            P("dp", None),
            P("dp"),
        ),
        out_specs=(P("section", "dp", None, None), P("section", "dp", None, None), P("section")),
        check_vma=False,
    )
```
